16 devices in a mesh: dp: 2 (over y, z), sp: 8 (over x, core).
Axes of the slice: x: 4, y: 2, z: 1, core: 2. Of those that a mesh axis runs over, the one named last changes fastest.
The devices are a block of a 4x4x8 slice.
Arguments:
- x: bfloat16 [2048, 6144], P(('dp', 'sp')), parts along dimension 0
- wq: bfloat16 [6144, 6144], replicated
- wk: bfloat16 [6144, 1024], replicated
- wv: bfloat16 [6144, 1024], replicated
- wo: bfloat16 [6144, 6144], replicated
- idx: int32 [2048, 4], P(('dp', 'sp')), parts along dimension 0
- probs: float32 [2048, 16], P(('dp', 'sp')), parts along dimension 0
Outputs:
- output 1: bfloat16 [2048, 6144], P(('dp', 'sp')), parts along dimension 0
- output 2: bfloat16 [32, 512, 6144], P(('dp', 'sp')), parts along dimension 0
There are 2 independent parts. The reference program is written for one: setup_inputs(seed, part) draws one part's arguments, and reference() takes and returns one part's arrays. A program takes and returns all parts, laid end to end along the dimension named above; an argument that names none is the same for every part.
All inputs are finite; a program needn't handle non-finite values.
Results may differ from the reference program's by a relative error of at most 0.00215937.
Values are sent between devices in bfloat16 or wider.
A program may use at most 768 MiB of HBM per device.

```python
import math
import jax
import jax.numpy as jnp
from jax import lax

H = 6144
HEADS = 48
KV_HEADS = 8
HEAD = 128
EXPERTS = 16
TOP = 4
SEQ = 1024
GROUP = 8
CAP = 64
ROPE_BASE = 1000000.0
QBLK = min(SEQ, 128)


def setup_inputs(seed: int = 0, part: int = 0) -> dict:
    key = jax.random.key(seed)
    kw = jax.random.split(key, 4)
    kd = jax.random.split(jax.random.fold_in(key, part), 3)
    ke = jax.random.split(jax.random.fold_in(jax.random.fold_in(key, part), 7), 2)
    sq = math.sqrt(math.log(max(SEQ / 16.0, 2.0)))
    x = jax.random.normal(kd[0], (SEQ, H), jnp.float32)
    wq = jax.random.normal(kw[0], (H, HEADS * HEAD), jnp.float32) * (sq / math.sqrt(H))
    wk = jax.random.normal(kw[1], (H, KV_HEADS * HEAD), jnp.float32) * (1.0 / math.sqrt(H))
    wv = jax.random.normal(kw[2], (H, KV_HEADS * HEAD), jnp.float32) * (1.0 / math.sqrt(H))
    wo = jax.random.normal(kw[3], (HEADS * HEAD, H), jnp.float32) * (1.0 / math.sqrt(HEADS * HEAD))
    normal_sum = jnp.sum(jax.random.randint(ke[0], (12, EXPERTS), 0, 256, jnp.int32), axis=0) * 2 - 12 * 255
    quarter_log = jnp.clip((normal_sum * 35) >> 11, -28, 28) + 28
    shift_part = (quarter_log >> 2).astype(jnp.uint32)
    mantissa = (8 - (quarter_log & 3)).astype(jnp.uint32)
    wait_time = ((jax.random.bits(ke[1], (SEQ, EXPERTS), jnp.uint32) >> 5) * mantissa[None, :]) >> shift_part[None, :]
    idx = jnp.argsort(wait_time, axis=1)[:, :TOP].astype(jnp.int32)
    probs = jax.nn.softmax(jax.random.normal(kd[2], (SEQ, EXPERTS), jnp.float32), axis=1)
    return {"x": x.astype(jnp.bfloat16), "wq": wq.astype(jnp.bfloat16), "wk": wk.astype(jnp.bfloat16), "wv": wv.astype(jnp.bfloat16), "wo": wo.astype(jnp.bfloat16), "idx": idx, "probs": probs}


def rope(t, pos):
    half = HEAD // 2
    inv = ROPE_BASE ** (-jnp.arange(half, dtype=jnp.float32) * (2.0 / HEAD))
    ang = pos.astype(jnp.float32)[:, None] * inv[None, :]
    c = jnp.cos(ang)[:, None, :]
    s = jnp.sin(ang)[:, None, :]
    a = t[..., :half]
    b = t[..., half:]
    return jnp.concatenate([a * c - b * s, b * c + a * s], axis=-1)


def reference(x, wq, wk, wv, wo, idx, probs):
    m = HEADS // KV_HEADS
    pos = jnp.arange(SEQ)
    q = rope(jnp.dot(x, wq, preferred_element_type=jnp.float32).reshape(SEQ, HEADS, HEAD), pos).astype(jnp.bfloat16)
    k = rope(jnp.dot(x, wk, preferred_element_type=jnp.float32).reshape(SEQ, KV_HEADS, HEAD), pos).astype(jnp.bfloat16)
    v = jnp.dot(x, wv, preferred_element_type=jnp.float32).astype(jnp.bfloat16).reshape(SEQ, KV_HEADS, HEAD)
    qg = q.reshape(SEQ, KV_HEADS, m, HEAD).transpose(1, 2, 0, 3)
    kg = k.transpose(1, 0, 2)
    vg = v.transpose(1, 0, 2)
    nb = SEQ // QBLK
    scale = 1.0 / math.sqrt(HEAD)

    def group(a):
        qh, kh, vh = a
        qs = qh.reshape(m, nb, QBLK, HEAD).transpose(1, 0, 2, 3)
        kf = kh.astype(jnp.float32)
        vf = vh.astype(jnp.float32)

        def block(b):
            qq, j = b
            sc = jnp.einsum("iqd,kd->iqk", qq.astype(jnp.float32), kf) * scale
            qpos = j * QBLK + jnp.arange(QBLK)
            keep = pos[None, :] <= qpos[:, None]
            sc = jnp.where(keep[None], sc, -jnp.inf)
            p = jax.nn.softmax(sc, axis=-1).astype(jnp.bfloat16)
            return jnp.einsum("iqk,kd->iqd", p.astype(jnp.float32), vf).astype(jnp.bfloat16)

        ob = lax.map(block, (qs, jnp.arange(nb)))
        return ob.transpose(1, 0, 2, 3).reshape(m, SEQ, HEAD)

    o = lax.map(group, (qg, kg, vg))
    o = o.transpose(2, 0, 1, 3).reshape(SEQ, HEADS * HEAD)
    h = (x.astype(jnp.float32) + jnp.dot(o, wo, preferred_element_type=jnp.float32)).astype(jnp.bfloat16)

    sd = SEQ // GROUP
    sel = jnp.take_along_axis(probs, idx, axis=1)
    w = sel / jnp.sum(sel, axis=1, keepdims=True)
    e = idx.reshape(GROUP, sd * TOP)
    hot = (e[:, :, None] == jnp.arange(EXPERTS)[None, None, :]).astype(jnp.int32)
    rank = jnp.sum(jnp.cumsum(hot, axis=1) * hot, axis=2) - 1
    dest = e * (GROUP * CAP) + jnp.arange(GROUP)[:, None] * CAP + rank
    dest = jnp.where(rank < CAP, dest, EXPERTS * GROUP * CAP).reshape(SEQ * TOP)
    rows = (w[:, :, None] * h[:, None, :].astype(jnp.float32)).astype(jnp.bfloat16).reshape(SEQ * TOP, H)
    buf = jnp.zeros((EXPERTS * GROUP * CAP, H), jnp.bfloat16).at[dest].set(rows, mode="drop")
    return h, buf.reshape(EXPERTS, GROUP * CAP, H)
```

```python
import functools
import math
import numpy as np
import jax
import jax.numpy as jnp
from jax import lax
from jax.experimental import pallas as pl
from jax.experimental.pallas import tpu as pltpu
from jax.sharding import PartitionSpec as P

HEAD = 128
ROPE_BASE = 1000000.0
CORES = 2
COL = 256
F32 = jnp.float32
BF16 = jnp.bfloat16
MESH = pl.DeviceIdType.MESH


def rope_table(length):
    inv = ROPE_BASE ** (-np.arange(HEAD // 2, dtype=np.float64) * (2.0 / HEAD))
    ang = np.arange(length, dtype=np.float64)[:, None] * inv[None, :]
    c, s = np.cos(ang), np.sin(ang)
    return np.stack([np.concatenate([c, c], 1), np.concatenate([-s, s], 1)]).astype(np.float32)


def block_kernel(n, kvh, m, nb, x_ref, wq_ref, wk_ref, wv_ref, wo_ref, idx_ref, probs_ref, rope_ref,
                 hg_ref, tw_ref,
                 xf, wbuf, cs, kvb, qt, of, ho, st, tw_own,
                 w_sem, x_sem, tws_sem, twr_sem, kvs_sem, kvf_sem, kvr_sem, os_sem, or_sem,
                 hl_sem, hs_sem, hf_sem, hp_sem, hr_sem, pr_sem):
    sd, hid = x_ref.shape
    chips = n // CORES
    ct = CORES * sd
    heads_c = kvh // CORES
    nk = heads_c * HEAD // COL
    nq = heads_c * m * HEAD // COL
    no = hid // CORES // COL
    hpc = COL // HEAD
    me = lax.axis_index("sp")
    chip = lax.div(me, CORES)
    core = lax.rem(me, CORES)
    partner = me + 1 - 2 * core
    right = lax.rem(me + CORES, n)
    left = lax.rem(me + n - CORES, n)
    rchip = lax.rem(chip + 1, chips)
    lchip = lax.rem(chip + chips - 1, chips)
    fchip = lax.rem(chip + 2, chips)

    def ds(i, size):
        return pl.ds(pl.multiple_of(i, size), size)

    def wcopy(src, col0, slot):
        return pltpu.make_async_copy(src.at[:, ds(col0, COL)], wbuf.at[slot], w_sem.at[slot])

    def k_copy(i, slot):
        return wcopy(wk_ref, core * (heads_c * HEAD) + i * COL, slot)

    def v_copy(i, slot):
        return wcopy(wv_ref, core * (heads_c * HEAD) + i * COL, slot)

    def q_copy(i, slot):
        return wcopy(wq_ref, core * (nq * COL) + i * COL, slot)

    def o_copy(i, slot):
        return wcopy(wo_ref, core * (no * COL) + i * COL, slot)

    base_q = 2 * nk
    for i in range(nk):
        k_copy(i, 2 * i).start()
        v_copy(i, 2 * i + 1).start()
    own_x = pltpu.make_async_copy(x_ref, xf.at[ds(core * sd, sd)], x_sem.at[2])
    own_x.start()
    rope_cp = pltpu.make_async_copy(rope_ref.at[:, ds(chip * ct, ct)], cs, x_sem.at[3])
    rope_cp.start()
    for i in range(nb - base_q):
        q_copy(i, base_q + i).start()

    barrier = pltpu.get_barrier_semaphore()

    @pl.loop(1, n)
    def _(off):
        pl.semaphore_signal(barrier, inc=1, device_id={"sp": lax.rem(me + off, n)}, device_id_type=MESH)

    pl.semaphore_wait(barrier, n - 1)

    def remote(src, dst, ssem, rsem, dev):
        return pltpu.make_async_remote_copy(src_ref=src, dst_ref=dst, send_sem=ssem, recv_sem=rsem,
                                            device_id={"sp": dev}, device_id_type=MESH)

    x_send = remote(x_ref, xf.at[ds(core * sd, sd)], x_sem.at[0], x_sem.at[1], partner)
    x_send.start()

    ne = probs_ref.shape[1]
    top = idx_ref.shape[1]
    per = ne // n
    cap = 2 * sd * top // ne
    probs = probs_ref[...]
    ei = lax.broadcasted_iota(jnp.int32, (sd, ne), 1)
    mine = jnp.zeros((sd, ne), F32)
    tot = jnp.zeros((sd, 1), F32)
    for c in range(top):
        hot = idx_ref[:, c:c + 1] == ei
        mine = jnp.where(hot, 1.0, mine)
        sel = jnp.sum(jnp.where(hot, probs, 0.0), axis=1, keepdims=True)
        tot = sel if c == 0 else tot + sel
    gate = probs / tot
    low = (lax.broadcasted_iota(jnp.int32, (sd, sd), 1) < lax.broadcasted_iota(jnp.int32, (sd, sd), 0))
    rank = jnp.dot(jnp.where(low, 1.0, 0.0).astype(BF16), mine.astype(BF16), preferred_element_type=F32)
    rank = jnp.where(mine > 0.5, rank, -1.0)
    rows = per * cap
    lane = lax.broadcasted_iota(jnp.int32, (sd, rows), 1)
    tok1 = (lax.broadcasted_iota(jnp.int32, (sd, rows), 0) + 1).astype(F32)
    sub = lax.broadcasted_iota(jnp.int32, (8, rows), 0)
    for d in range(n):
        rk = jnp.broadcast_to(rank[:, per * d:per * d + 1], (sd, rows))
        gt = jnp.broadcast_to(gate[:, per * d:per * d + 1], (sd, rows))
        for k in range(1, per):
            rk = jnp.where(lane >= k * cap, rank[:, per * d + k:per * d + k + 1], rk)
            gt = jnp.where(lane >= k * cap, gate[:, per * d + k:per * d + k + 1], gt)
        hit = rk == lax.rem(lane, cap).astype(F32)
        t_row = jnp.sum(jnp.where(hit, tok1, 0.0), axis=0, keepdims=True) - 1.0
        w_row = jnp.sum(jnp.where(hit, gt, 0.0), axis=0, keepdims=True)
        tw_own[d] = jnp.where(sub == 0, t_row, jnp.where(sub == 1, w_row, 0.0))
    tw_own_local = pltpu.make_async_copy(tw_own.at[me], tw_ref.at[me], twr_sem.at[me])
    tw_own_local.start()

    def tw_send(off):
        d = lax.rem(me + off, n)
        return remote(tw_own.at[d], tw_ref.at[me], tws_sem.at[d], twr_sem.at[me], d)

    @pl.loop(1, n)
    def _(off):
        tw_send(off).start()

    own_x.wait()
    rope_cp.wait()
    x_send.wait_recv()

    def rope(t):
        return t * cs[0] + pltpu.roll(t, HEAD // 2, 1) * cs[1]

    def kv_send(h, side):
        dev = right if side == 0 else left
        return remote(kvb.at[chip, h], kvb.at[chip, h], kvs_sem.at[side, h], kvr_sem.at[side, h], dev)

    def kv_forward(h):
        even = h % 2 == 0
        src = lchip if even else rchip
        dev = right if even else left
        return remote(kvb.at[src, h], kvb.at[src, h], kvf_sem.at[h], kvr_sem.at[2, h], dev)

    @pl.loop(0, nk)
    def _(i):
        k_copy(0, 2 * i).wait()
        acc = jnp.dot(xf[...], wbuf[2 * i], preferred_element_type=F32)
        for hh in range(hpc):
            kvb[chip, hpc * i + hh, 0:ct] = rope(acc[:, hh * HEAD:(hh + 1) * HEAD]).astype(BF16)
        v_copy(0, 2 * i + 1).wait()
        acc = jnp.dot(xf[...], wbuf[2 * i + 1], preferred_element_type=F32)
        for hh in range(hpc):
            vt = acc[:, hh * HEAD:(hh + 1) * HEAD].T.astype(BF16)
            for b in range(ct // HEAD):
                kvb[chip, hpc * i + hh, ct + b * HEAD:ct + (b + 1) * HEAD] = vt[:, b * HEAD:(b + 1) * HEAD]
        for hh in range(hpc):
            for side in range(2):
                kv_send(hpc * i + hh, side).start()
        q_copy(nb - base_q + 2 * i, 2 * i).start()
        q_copy(nb - base_q + 2 * i + 1, 2 * i + 1).start()

    fwd_at = [nq * 5 // 12 + (nq * 2 // 12) * h for h in range(heads_c)]

    @pl.loop(0, nq)
    def _(i):
        slot = lax.rem(base_q + i, nb)
        q_copy(0, slot).wait()
        acc = jnp.dot(xf[...], wbuf[slot], preferred_element_type=F32)
        for hh in range(hpc):
            qt[hpc * i + hh] = rope(acc[:, hh * HEAD:(hh + 1) * HEAD]).T.astype(BF16)
        o_copy(i, slot).start()
        for h in range(heads_c):
            @pl.when(i == fwd_at[h])
            def _(h=h):
                kv_send(h, h % 2).wait_recv()
                kv_forward(h).start()

    ex = math.log2(math.e) / math.sqrt(HEAD)
    key_i = lax.broadcasted_iota(jnp.int32, (ct, ct), 0)
    qry_i = lax.broadcasted_iota(jnp.int32, (ct, ct), 1)

    def head(nc, h, g):
        q = qt[h * m + g]
        mx = None
        for j in range(nc):
            s = jnp.dot(kvb[j, h, 0:ct], q, preferred_element_type=F32)
            if j == nc - 1:
                s = jnp.where(key_i <= qry_i, s, -jnp.inf)
            st[j] = s
            sm = jnp.max(s, axis=0, keepdims=True)
            mx = sm if mx is None else jnp.maximum(mx, sm)
        tot = None
        for j in range(nc):
            p = jnp.exp2((st[j] - mx) * ex)
            st[j] = p
            ps = jnp.sum(p, axis=0, keepdims=True)
            tot = ps if tot is None else tot + ps
        inv = 1.0 / tot
        o = None
        for j in range(nc):
            vt = jnp.concatenate([kvb[j, h, ct + b * HEAD:ct + (b + 1) * HEAD] for b in range(ct // HEAD)], axis=1)
            oj = jnp.dot(vt, (st[j] * inv).astype(BF16), preferred_element_type=F32)
            o = oj if o is None else o + oj
        of[core * heads_c + h, :, ds(g * HEAD, HEAD)] = o.T.astype(BF16)

    def o_send(h):
        return remote(of.at[core * heads_c + h], of.at[core * heads_c + h], os_sem.at[h], or_sem.at[h], partner)

    @pl.loop(0, heads_c)
    def _(h):
        even = lax.rem(h, 2) == 0
        @pl.when(even)
        def _():
            kv_send(h, 1).wait_recv()

        @pl.when(jnp.logical_not(even))
        def _():
            kv_send(h, 0).wait_recv()

        remote(kvb.at[fchip, h], kvb.at[fchip, h], kvf_sem.at[h], kvr_sem.at[2, h], right).wait_recv()
        for nc in range(1, chips + 1):
            @pl.when(chip == nc - 1)
            def _(nc=nc):
                @pl.loop(0, m)
                def _(g):
                    head(nc, h, g)
        o_send(h).start()

    @pl.loop(0, heads_c)
    def _(h):
        pltpu.make_async_copy(of.at[(1 - core) * heads_c + h], of.at[(1 - core) * heads_c + h], or_sem.at[h]).wait()

    def place(c, j, who):
        return hg_ref.at[c * no + j, ds(who * ct, ct)]

    def h_local(j):
        return pltpu.make_async_copy(ho.at[j], place(core, j, chip), hl_sem.at[j])

    def h_send(j, side):
        dev = (right, left, partner)[side]
        return remote(ho.at[j], place(core, j, chip), hs_sem.at[side, j],
                      hr_sem.at[side, j] if side < 2 else pr_sem.at[0, j], dev)

    def h_forward(j, side):
        src = (lchip, rchip)[side]
        dev = (right, left)[side]
        return remote(place(core, j, src), place(core, j, src), hf_sem.at[j], hr_sem.at[2, j], dev)

    def h_pass(j, k):
        src = (None, lchip, rchip, fchip)[k]
        return remote(place(core, j, src), place(core, j, src), hp_sem.at[k - 1, j], pr_sem.at[k, j], partner)

    group = m * HEAD

    @pl.loop(0, no)
    def _(j):
        slot = lax.rem(base_q + nq + j, nb)
        o_copy(0, slot).wait()
        acc = None
        for g in range(kvh):
            t = jnp.dot(of[g], wbuf[slot, g * group:(g + 1) * group], preferred_element_type=F32)
            acc = t if acc is None else acc + t
        xs = xf[:, ds(core * (no * COL) + j * COL, COL)].astype(F32)
        ho[j] = (xs + acc).astype(BF16)
        h_send(j, 0).start()
        h_send(j, 1).start()
        h_send(j, 2).start()
        h_local(j).start()

    @pl.loop(0, no)
    def _(j):
        h_send(j, 0).wait_recv()
        even = lax.rem(j, 2) == 0

        @pl.when(even)
        def _():
            h_forward(j, 0).start()

        h_pass(j, 1).start()
        h_send(j, 1).wait_recv()

        @pl.when(jnp.logical_not(even))
        def _():
            h_forward(j, 1).start()

        h_pass(j, 2).start()

    @pl.loop(0, no)
    def _(j):
        h_forward(j, 0).wait_recv()
        h_pass(j, 3).start()

    @pl.loop(0, no)
    def _(j):
        for side in range(3):
            h_send(j, side).wait_send()
        h_local(j).wait()
        h_forward(j, 0).wait_send()
        for k in range(1, 4):
            h_pass(j, k).wait_send()
        for k in range(4):
            pltpu.make_async_copy(ho.at[j], place(core, j, chip), pr_sem.at[k, j]).wait()

    for h in range(heads_c):
        o_send(h).wait_send()
        kv_forward(h).wait_send()
        for side in range(2):
            kv_send(h, side).wait_send()
    x_send.wait_send()
    tw_own_local.wait()

    @pl.loop(1, n)
    def _(off):
        tw_send(off).wait_send()
        d = lax.rem(me + off, n)
        pltpu.make_async_copy(tw_own.at[d], tw_ref.at[d], twr_sem.at[d]).wait()


def build_kernel(n, me_ref, hg_ref, tw_ref, h_ref, buf_ref, pick, wcol):
    nch, toks, col = hg_ref.shape
    sd = h_ref.shape[0]
    per = buf_ref.shape[0]
    rows = tw_ref.shape[2]
    cap = rows // per

    @pl.when(pl.program_id(0) == 0)
    def _():
        li = lax.broadcasted_iota(jnp.int32, (rows, sd), 1).astype(F32)
        for s in range(n):
            t = jnp.broadcast_to(tw_ref[s, 0:1, :], (sd, rows)).T
            pick[s] = jnp.where(t == li, 1.0, 0.0).astype(BF16)
            wcol[s] = jnp.broadcast_to(tw_ref[s, 1:2, :], (sd, rows)).T

    for c in range(nch):
        h_ref[:, c * col:(c + 1) * col] = hg_ref[c, pl.ds(pl.multiple_of(me_ref[0] * sd, sd), sd), :]
        for s in range(n):
            r = jnp.dot(pick[s], hg_ref[c, s * sd:(s + 1) * sd, :], preferred_element_type=F32)
            w = jnp.concatenate([wcol[s]] * (col // sd), axis=1)
            r = (w * r).astype(BF16)
            for e in range(per):
                buf_ref[e, s * cap:(s + 1) * cap, c * col:(c + 1) * col] = r[e * cap:(e + 1) * cap]


def solution(mesh):
    n = mesh.shape["sp"]
    row = P(("dp", "sp"), None)
    full = P(None, None)

    def local(x, wq, wk, wv, wo, idx, probs):
        sd, hid = x.shape
        heads = wq.shape[1] // HEAD
        kvh = wk.shape[1] // HEAD
        m = heads // kvh
        ne = probs.shape[1]
        per = ne // n
        cap = 2 * sd * idx.shape[1] // ne
        rows = per * cap
        chips = n // CORES
        ct = CORES * sd
        hc = kvh // CORES
        no = hid // CORES // COL
        nq = hc * m * HEAD // COL
        nb = 12
        dma = pltpu.SemaphoreType.DMA
        any_ = pl.BlockSpec(memory_space=pl.ANY)
        vm = pl.BlockSpec(memory_space=pltpu.VMEM)
        hg, tw = pl.pallas_call(
            functools.partial(block_kernel, n, kvh, m, nb),
            out_shape=(jax.ShapeDtypeStruct((CORES * no, n * sd, COL), BF16),
                       jax.ShapeDtypeStruct((n, 8, rows), F32)),
            in_specs=[any_, any_, any_, any_, any_, vm, vm, any_],
            out_specs=(any_, any_),
            scratch_shapes=[
                pltpu.VMEM((ct, hid), BF16),
                pltpu.VMEM((nb, hid, COL), BF16),
                pltpu.VMEM((2, ct, HEAD), F32),
                pltpu.VMEM((chips, hc, 2 * ct, HEAD), BF16),
                pltpu.VMEM((hc * m, HEAD, ct), BF16),
                pltpu.VMEM((kvh, ct, m * HEAD), BF16),
                pltpu.VMEM((no, ct, COL), BF16),
                pltpu.VMEM((chips, ct, ct), F32),
                pltpu.VMEM((n, 8, rows), F32),
                dma((nb,)), dma((4,)), dma((n,)), dma((n,)),
                dma((2, hc)), dma((hc,)), dma((3, hc)), dma((hc,)), dma((hc,)),
                dma((no,)), dma((3, no)), dma((no,)), dma((3, no)), dma((3, no)), dma((4, no)),
            ],
            compiler_params=pltpu.CompilerParams(collective_id=0, has_side_effects=True,
                                                 vmem_limit_bytes=66_000_000),
        )(x, wq, wk, wv, wo, idx, probs, jnp.asarray(rope_table(n * sd)))

        step = 4
        me = lax.axis_index("sp").astype(jnp.int32).reshape(1)
        h, buf = pl.pallas_call(
            functools.partial(build_kernel, n),
            out_shape=(jax.ShapeDtypeStruct((sd, hid), BF16),
                       jax.ShapeDtypeStruct((per, n * cap, hid), BF16)),
            grid_spec=pltpu.PrefetchScalarGridSpec(
                num_scalar_prefetch=1, grid=(CORES * no // step,),
                in_specs=[pl.BlockSpec((step, n * sd, COL), lambda i, r: (i, 0, 0)),
                          pl.BlockSpec((n, 8, rows), lambda i, r: (0, 0, 0))],
                out_specs=(pl.BlockSpec((sd, step * COL), lambda i, r: (0, i)),
                           pl.BlockSpec((per, n * cap, step * COL), lambda i, r: (0, 0, i))),
                scratch_shapes=[pltpu.VMEM((n, rows, sd), BF16), pltpu.VMEM((n, rows, sd), F32)]),
        )(me, hg, tw)
        return h, buf

    return jax.shard_map(local, mesh=mesh, in_specs=(row, full, full, full, full, row, row), out_specs=(row, P(("dp", "sp"), None, None)), check_vma=False)
```

```python
import functools
import math
import numpy as np
import jax
import jax.numpy as jnp
from jax import lax
from jax.experimental import pallas as pl
from jax.experimental.pallas import tpu as pltpu
from jax.sharding import PartitionSpec as P

HEAD = 128
ROPE_BASE = 1000000.0
CORES = 2
COL = 256
F32 = jnp.float32
BF16 = jnp.bfloat16
MESH = pl.DeviceIdType.MESH


def rope_table(length):
    inv = ROPE_BASE ** (-np.arange(HEAD // 2, dtype=np.float64) * (2.0 / HEAD))
    ang = np.arange(length, dtype=np.float64)[:, None] * inv[None, :]
    c, s = np.cos(ang), np.sin(ang)
    return np.stack([np.concatenate([c, c], 1), np.concatenate([-s, s], 1)]).astype(np.float32)


def block_kernel(n, kvh, m, nb, x_ref, wq_ref, wk_ref, wv_ref, wo_ref, idx_ref, probs_ref, rope_ref,
                 hg_ref, tw_ref,
                 xf, wbuf, cs, kvb, qt, of, ho, st, accs, tw_own, idx_v, probs_v,
                 w_sem, x_sem, tws_sem, twr_sem, kvs_sem, kvf_sem, kvr_sem, os_sem, or_sem,
                 hl_sem, hs_sem, hf_sem, hp_sem, hr_sem, pr_sem):
    sd, hid = x_ref.shape
    chips = n // CORES
    ct = CORES * sd
    heads_c = kvh // CORES
    nk = heads_c * HEAD // COL
    nq = heads_c * m * HEAD // COL
    no = hid // CORES // COL
    hpc = COL // HEAD
    me = lax.axis_index("sp")
    chip = lax.div(me, CORES)
    core = lax.rem(me, CORES)
    partner = me + 1 - 2 * core
    right = lax.rem(me + CORES, n)
    left = lax.rem(me + n - CORES, n)
    rchip = lax.rem(chip + 1, chips)
    lchip = lax.rem(chip + chips - 1, chips)
    fchip = lax.rem(chip + 2, chips)

    def ds(i, size):
        return pl.ds(pl.multiple_of(i, size), size)

    def wcopy(src, col0, slot):
        return pltpu.make_async_copy(src.at[:, ds(col0, COL)], wbuf.at[slot], w_sem.at[slot])

    def k_copy(i, slot):
        return wcopy(wk_ref, core * (heads_c * HEAD) + i * COL, slot)

    def v_copy(i, slot):
        return wcopy(wv_ref, core * (heads_c * HEAD) + i * COL, slot)

    def q_copy(i, slot):
        return wcopy(wq_ref, core * (nq * COL) + i * COL, slot)

    def o_copy(i, slot):
        return wcopy(wo_ref, core * (no * COL) + i * COL, slot)

    base_q = 2 * nk
    own_x = pltpu.make_async_copy(x_ref, xf.at[ds(core * sd, sd)], x_sem.at[2])
    own_x.start()
    rope_cp = pltpu.make_async_copy(rope_ref.at[:, ds(chip * ct, ct)], cs, x_sem.at[3])
    rope_cp.start()
    idx_cp = pltpu.make_async_copy(idx_ref, idx_v, x_sem.at[4])
    idx_cp.start()
    probs_cp = pltpu.make_async_copy(probs_ref, probs_v, x_sem.at[5])
    probs_cp.start()
    for i in range(nk):
        k_copy(i, 2 * i).start()
        v_copy(i, 2 * i + 1).start()

    barrier = pltpu.get_barrier_semaphore()

    @pl.loop(1, n)
    def _(off):
        pl.semaphore_signal(barrier, inc=1, device_id={"sp": lax.rem(me + off, n)}, device_id_type=MESH)

    pl.semaphore_wait(barrier, n - 1)

    def remote(src, dst, ssem, rsem, dev):
        return pltpu.make_async_remote_copy(src_ref=src, dst_ref=dst, send_sem=ssem, recv_sem=rsem,
                                            device_id={"sp": dev}, device_id_type=MESH)

    x_send = remote(x_ref, xf.at[ds(core * sd, sd)], x_sem.at[0], x_sem.at[1], partner)
    x_send.start()
    for i in range(nb - base_q):
        q_copy(i, base_q + i).start()

    ne = probs_ref.shape[0]
    top = idx_ref.shape[0]
    per = ne // n
    cap = 2 * sd * top // ne
    idx_cp.wait()
    probs_cp.wait()
    probs = probs_v[...]
    ei = lax.broadcasted_iota(jnp.int32, (ne, sd), 0)
    mine = jnp.zeros((ne, sd), F32)
    tot = None
    for c in range(top):
        hot = idx_v[c:c + 1, :] == ei
        mine = jnp.where(hot, 1.0, mine)
        sel = jnp.sum(jnp.where(hot, probs, 0.0), axis=0, keepdims=True)
        tot = sel if tot is None else tot + sel
    low = (lax.broadcasted_iota(jnp.int32, (sd, sd), 0) < lax.broadcasted_iota(jnp.int32, (sd, sd), 1))
    rank = jnp.dot(mine.astype(BF16), jnp.where(low, 1.0, 0.0).astype(BF16), preferred_element_type=F32)
    rank = jnp.where(mine > 0.5, rank, -1.0).T
    gate = (probs / tot).T
    rows = per * cap
    lane = lax.broadcasted_iota(jnp.int32, (sd, rows), 1)
    tok1 = (lax.broadcasted_iota(jnp.int32, (sd, rows), 0) + 1).astype(F32)
    sub = lax.broadcasted_iota(jnp.int32, (8, rows), 0)
    for d in range(n):
        rk = jnp.broadcast_to(rank[:, per * d:per * d + 1], (sd, rows))
        gt = jnp.broadcast_to(gate[:, per * d:per * d + 1], (sd, rows))
        for k in range(1, per):
            rk = jnp.where(lane >= k * cap, rank[:, per * d + k:per * d + k + 1], rk)
            gt = jnp.where(lane >= k * cap, gate[:, per * d + k:per * d + k + 1], gt)
        hit = rk == lax.rem(lane, cap).astype(F32)
        t_row = jnp.sum(jnp.where(hit, tok1, 0.0), axis=0, keepdims=True) - 1.0
        w_row = jnp.sum(jnp.where(hit, gt, 0.0), axis=0, keepdims=True)
        tw_own[d] = jnp.where(sub == 0, t_row, jnp.where(sub == 1, w_row, 0.0))
    tw_own_local = pltpu.make_async_copy(tw_own.at[me], tw_ref.at[me], twr_sem.at[me])
    tw_own_local.start()

    def tw_send(off):
        d = lax.rem(me + off, n)
        return remote(tw_own.at[d], tw_ref.at[me], tws_sem.at[d], twr_sem.at[me], d)

    @pl.loop(1, n)
    def _(off):
        tw_send(off).start()

    own_x.wait()
    rope_cp.wait()
    x_send.wait_recv()

    def rope(t):
        return t * cs[0] + pltpu.roll(t, HEAD // 2, 1) * cs[1]

    def kv_send(h, side):
        dev = right if side == 0 else left
        return remote(kvb.at[chip, h], kvb.at[chip, h], kvs_sem.at[side, h], kvr_sem.at[side, h], dev)

    def kv_forward(h):
        even = h % 2 == 0
        src = lchip if even else rchip
        dev = right if even else left
        return remote(kvb.at[src, h], kvb.at[src, h], kvf_sem.at[h], kvr_sem.at[2, h], dev)

    @pl.loop(0, nk)
    def _(i):
        k_copy(0, 2 * i).wait()
        v_copy(0, 2 * i + 1).wait()
        ka = jnp.dot(xf[...], wbuf[2 * i], preferred_element_type=F32)
        va = jnp.dot(xf[...], wbuf[2 * i + 1], preferred_element_type=F32)
        for hh in range(hpc):
            kvb[chip, hpc * i + hh, 0:ct] = rope(ka[:, hh * HEAD:(hh + 1) * HEAD]).astype(BF16)
        for hh in range(hpc):
            vt = va[:, hh * HEAD:(hh + 1) * HEAD].T.astype(BF16)
            for b in range(ct // HEAD):
                kvb[chip, hpc * i + hh, ct + b * HEAD:ct + (b + 1) * HEAD] = vt[:, b * HEAD:(b + 1) * HEAD]
        for hh in range(hpc):
            for side in range(2):
                kv_send(hpc * i + hh, side).start()
        q_copy(nb - base_q + 2 * i, 2 * i).start()
        q_copy(nb - base_q + 2 * i + 1, 2 * i + 1).start()

    def q_store(i):
        for hh in range(hpc):
            qt[i, :, hh * ct:(hh + 1) * ct] = rope(accs[:, hh * HEAD:(hh + 1) * HEAD]).T.astype(BF16)

    accs[...] = jnp.zeros_like(accs)
    fwd_at = [nq * 5 // 12 + (nq * 2 // 12) * h for h in range(heads_c)]

    @pl.loop(0, nq)
    def _(i):
        slot = lax.rem(base_q + i, nb)
        q_copy(0, slot).wait()
        q_store(jnp.maximum(i - 1, 0))
        accs[...] = jnp.dot(xf[...], wbuf[slot], preferred_element_type=F32)
        o_copy(i, slot).start()
        for h in range(heads_c):
            @pl.when(i == fwd_at[h])
            def _(h=h):
                kv_send(h, h % 2).wait_recv()
                kv_forward(h).start()

    q_store(nq - 1)
    ex = math.log2(math.e) / math.sqrt(HEAD)
    wide = hpc * ct
    key_i = lax.broadcasted_iota(jnp.int32, (ct, wide), 0)
    qry_i = lax.rem(lax.broadcasted_iota(jnp.int32, (ct, wide), 1), ct)

    def attend(nc, h, g):
        q = qt[h * (m // hpc) + g]
        mx = None
        for j in range(nc):
            s = jnp.dot(kvb[j, h, 0:ct], q, preferred_element_type=F32)
            if j == nc - 1:
                s = jnp.where(key_i <= qry_i, s, -jnp.inf)
            st[j] = s
            sm = jnp.max(s, axis=0, keepdims=True)
            mx = sm if mx is None else jnp.maximum(mx, sm)
        tot = None
        for j in range(nc):
            p = jnp.exp2((st[j] - mx) * ex)
            st[j] = p
            ps = jnp.sum(p, axis=0, keepdims=True)
            tot = ps if tot is None else tot + ps
        inv = 1.0 / tot
        o = None
        for j in range(nc):
            vt = jnp.concatenate([kvb[j, h, ct + b * HEAD:ct + (b + 1) * HEAD] for b in range(ct // HEAD)], axis=1)
            oj = jnp.dot(vt, (st[j] * inv).astype(BF16), preferred_element_type=F32)
            o = oj if o is None else o + oj
        o = jnp.concatenate([o[:, k * ct:(k + 1) * ct].T for k in range(hpc)], axis=1)
        of[core * heads_c + h, :, ds(g * COL, COL)] = o.astype(BF16)

    def o_send(h):
        return remote(of.at[core * heads_c + h], of.at[core * heads_c + h], os_sem.at[h], or_sem.at[h], partner)

    @pl.loop(0, heads_c)
    def _(h):
        even = lax.rem(h, 2) == 0
        @pl.when(even)
        def _():
            kv_send(h, 1).wait_recv()

        @pl.when(jnp.logical_not(even))
        def _():
            kv_send(h, 0).wait_recv()

        remote(kvb.at[fchip, h], kvb.at[fchip, h], kvf_sem.at[h], kvr_sem.at[2, h], right).wait_recv()
        for nc in range(1, chips + 1):
            @pl.when(chip == nc - 1)
            def _(nc=nc):
                @pl.loop(0, m // hpc)
                def _(g):
                    attend(nc, h, g)
        o_send(h).start()

    @pl.loop(0, heads_c)
    def _(h):
        pltpu.make_async_copy(of.at[(1 - core) * heads_c + h], of.at[(1 - core) * heads_c + h], or_sem.at[h]).wait()

    def place(c, j, who):
        return hg_ref.at[c * no + j, ds(who * ct, ct)]

    def h_local(j):
        return pltpu.make_async_copy(ho.at[j], place(core, j, chip), hl_sem.at[j])

    def h_send(j, side):
        dev = (right, left, partner)[side]
        return remote(ho.at[j], place(core, j, chip), hs_sem.at[side, j],
                      hr_sem.at[side, j] if side < 2 else pr_sem.at[0, j], dev)

    def h_forward(j, side):
        src = (lchip, rchip)[side]
        dev = (right, left)[side]
        return remote(place(core, j, src), place(core, j, src), hf_sem.at[j], hr_sem.at[2, j], dev)

    def h_pass(j, k):
        src = (None, lchip, rchip, fchip)[k]
        return remote(place(core, j, src), place(core, j, src), hp_sem.at[k - 1, j], pr_sem.at[k, j], partner)

    group = m * HEAD

    @pl.loop(0, no)
    def _(j):
        slot = lax.rem(base_q + nq + j, nb)
        o_copy(0, slot).wait()
        acc = None
        for g in range(kvh):
            t = jnp.dot(of[g], wbuf[slot, g * group:(g + 1) * group], preferred_element_type=F32)
            acc = t if acc is None else acc + t
        xs = xf[:, ds(core * (no * COL) + j * COL, COL)].astype(F32)
        ho[j] = (xs + acc).astype(BF16)
        h_send(j, 0).start()
        h_send(j, 1).start()
        h_send(j, 2).start()
        h_local(j).start()

    @pl.loop(0, no)
    def _(j):
        h_send(j, 0).wait_recv()
        even = lax.rem(j, 2) == 0

        @pl.when(even)
        def _():
            h_forward(j, 0).start()

        h_pass(j, 1).start()
        h_send(j, 1).wait_recv()

        @pl.when(jnp.logical_not(even))
        def _():
            h_forward(j, 1).start()

        h_pass(j, 2).start()

    @pl.loop(0, no)
    def _(j):
        h_forward(j, 0).wait_recv()
        h_pass(j, 3).start()

    @pl.loop(0, no)
    def _(j):
        for side in range(3):
            h_send(j, side).wait_send()
        h_local(j).wait()
        h_forward(j, 0).wait_send()
        for k in range(1, 4):
            h_pass(j, k).wait_send()
        for k in range(4):
            pltpu.make_async_copy(ho.at[j], place(core, j, chip), pr_sem.at[k, j]).wait()

    for h in range(heads_c):
        o_send(h).wait_send()
        kv_forward(h).wait_send()
        for side in range(2):
            kv_send(h, side).wait_send()
    x_send.wait_send()
    tw_own_local.wait()

    @pl.loop(1, n)
    def _(off):
        tw_send(off).wait_send()
        d = lax.rem(me + off, n)
        pltpu.make_async_copy(tw_own.at[d], tw_ref.at[d], twr_sem.at[d]).wait()


def build_kernel(n, me_ref, hg_ref, tw_ref, h_ref, buf_ref, pick, wcol):
    nch, toks, col = hg_ref.shape
    sd = h_ref.shape[0]
    per = buf_ref.shape[0]
    rows = tw_ref.shape[2]
    cap = rows // per

    @pl.when(pl.program_id(0) == 0)
    def _():
        li = lax.broadcasted_iota(jnp.int32, (rows, sd), 1).astype(F32)
        for s in range(n):
            t = jnp.broadcast_to(tw_ref[s, 0:1, :], (sd, rows)).T
            pick[s] = jnp.where(t == li, 1.0, 0.0).astype(BF16)
            wcol[s] = jnp.broadcast_to(tw_ref[s, 1:2, :], (sd, rows)).T

    for c in range(nch):
        h_ref[:, c * col:(c + 1) * col] = hg_ref[c, pl.ds(pl.multiple_of(me_ref[0] * sd, sd), sd), :]
        for s in range(n):
            r = jnp.dot(pick[s], hg_ref[c, s * sd:(s + 1) * sd, :], preferred_element_type=F32)
            w = jnp.concatenate([wcol[s]] * (col // sd), axis=1)
            r = (w * r).astype(BF16)
            for e in range(per):
                buf_ref[e, s * cap:(s + 1) * cap, c * col:(c + 1) * col] = r[e * cap:(e + 1) * cap]


def solution(mesh):
    n = mesh.shape["sp"]
    row = P(("dp", "sp"), None)
    full = P(None, None)

    def local(x, wq, wk, wv, wo, idx, probs):
        sd, hid = x.shape
        heads = wq.shape[1] // HEAD
        kvh = wk.shape[1] // HEAD
        m = heads // kvh
        ne = probs.shape[1]
        per = ne // n
        cap = 2 * sd * idx.shape[1] // ne
        rows = per * cap
        chips = n // CORES
        ct = CORES * sd
        hc = kvh // CORES
        no = hid // CORES // COL
        nq = hc * m * HEAD // COL
        nb = 12
        dma = pltpu.SemaphoreType.DMA
        any_ = pl.BlockSpec(memory_space=pl.ANY)
        hg, tw = pl.pallas_call(
            functools.partial(block_kernel, n, kvh, m, nb),
            out_shape=(jax.ShapeDtypeStruct((CORES * no, n * sd, COL), BF16),
                       jax.ShapeDtypeStruct((n, 8, rows), F32)),
            in_specs=[any_] * 8,
            out_specs=(any_, any_),
            scratch_shapes=[
                pltpu.VMEM((ct, hid), BF16),
                pltpu.VMEM((nb, hid, COL), BF16),
                pltpu.VMEM((2, ct, HEAD), F32),
                pltpu.VMEM((chips, hc, 2 * ct, HEAD), BF16),
                pltpu.VMEM((nq, HEAD, COL // HEAD * ct), BF16),
                pltpu.VMEM((kvh, ct, m * HEAD), BF16),
                pltpu.VMEM((no, ct, COL), BF16),
                pltpu.VMEM((chips, ct, COL // HEAD * ct), F32),
                pltpu.VMEM((ct, COL), F32),
                pltpu.VMEM((n, 8, rows), F32),
                pltpu.VMEM(idx.shape[::-1], jnp.int32),
                pltpu.VMEM(probs.shape[::-1], F32),
                dma((nb,)), dma((6,)), dma((n,)), dma((n,)),
                dma((2, hc)), dma((hc,)), dma((3, hc)), dma((hc,)), dma((hc,)),
                dma((no,)), dma((3, no)), dma((no,)), dma((3, no)), dma((3, no)), dma((4, no)),
            ],
            compiler_params=pltpu.CompilerParams(collective_id=0, has_side_effects=True,
                                                 vmem_limit_bytes=66_000_000),
        )(x, wq, wk, wv, wo, idx.T, probs.T, jnp.asarray(rope_table(n * sd)))

        step = 4
        me = lax.axis_index("sp").astype(jnp.int32).reshape(1)
        h, buf = pl.pallas_call(
            functools.partial(build_kernel, n),
            out_shape=(jax.ShapeDtypeStruct((sd, hid), BF16),
                       jax.ShapeDtypeStruct((per, n * cap, hid), BF16)),
            grid_spec=pltpu.PrefetchScalarGridSpec(
                num_scalar_prefetch=1, grid=(CORES * no // step,),
                in_specs=[pl.BlockSpec((step, n * sd, COL), lambda i, r: (i, 0, 0)),
                          pl.BlockSpec((n, 8, rows), lambda i, r: (0, 0, 0))],
                out_specs=(pl.BlockSpec((sd, step * COL), lambda i, r: (0, i)),
                           pl.BlockSpec((per, n * cap, step * COL), lambda i, r: (0, 0, i))),
                scratch_shapes=[pltpu.VMEM((n, rows, sd), BF16), pltpu.VMEM((n, rows, sd), F32)]),
        )(me, hg, tw)
        return h, buf

    return jax.shard_map(local, mesh=mesh, in_specs=(row, full, full, full, full, row, row), out_specs=(row, P(("dp", "sp"), None, None)), check_vma=False)
```

```python
import functools
import math
import numpy as np
import jax
import jax.numpy as jnp
from jax import lax
from jax.experimental import pallas as pl
from jax.experimental.pallas import tpu as pltpu
from jax.sharding import PartitionSpec as P

HEAD = 128
ROPE_BASE = 1000000.0
CORES = 2
COL = 256
F32 = jnp.float32
BF16 = jnp.bfloat16
MESH = pl.DeviceIdType.MESH


def rope_table(length):
    inv = ROPE_BASE ** (-np.arange(HEAD // 2, dtype=np.float64) * (2.0 / HEAD))
    ang = np.arange(length, dtype=np.float64)[:, None] * inv[None, :]
    c, s = np.cos(ang), np.sin(ang)
    return np.stack([np.concatenate([c, c], 1), np.concatenate([-s, s], 1)]).astype(np.float32)


def block_kernel(n, kvh, m, nb, x_ref, wq_ref, wk_ref, wv_ref, wo_ref, idx_ref, probs_ref, rope_ref,
                 hg_ref, pick_ref, wcol_ref,
                 xf, wbuf, cs, kvb, qt, of, ho, st, accs, tw_own, tw_all, idx_v, probs_v,
                 w_sem, x_sem, tws_sem, twr_sem, kvs_sem, kvf_sem, kvr_sem, os_sem, or_sem,
                 hl_sem, hs_sem, hf_sem, hp_sem, hr_sem, pr_sem):
    sd, hid = x_ref.shape
    chips = n // CORES
    ct = CORES * sd
    heads_c = kvh // CORES
    nk = heads_c * HEAD // COL
    nq = heads_c * m * HEAD // COL
    no = hid // CORES // COL
    hpc = COL // HEAD
    me = lax.axis_index("sp")
    chip = lax.div(me, CORES)
    core = lax.rem(me, CORES)
    partner = me + 1 - 2 * core
    right = lax.rem(me + CORES, n)
    left = lax.rem(me + n - CORES, n)
    rchip = lax.rem(chip + 1, chips)
    lchip = lax.rem(chip + chips - 1, chips)
    fchip = lax.rem(chip + 2, chips)

    def ds(i, size):
        return pl.ds(pl.multiple_of(i, size), size)

    def wcopy(src, col0, slot):
        return pltpu.make_async_copy(src.at[:, ds(col0, COL)], wbuf.at[slot], w_sem.at[slot])

    def k_copy(i, slot):
        return wcopy(wk_ref, core * (heads_c * HEAD) + i * COL, slot)

    def v_copy(i, slot):
        return wcopy(wv_ref, core * (heads_c * HEAD) + i * COL, slot)

    def q_copy(i, slot):
        return wcopy(wq_ref, core * (nq * COL) + i * COL, slot)

    def o_copy(i, slot):
        return wcopy(wo_ref, core * (no * COL) + i * COL, slot)

    base_q = 2 * nk

    def fetch(g):
        slot = lax.rem(g, nb)

        @pl.when(g < base_q + nq)
        def _():
            q_copy(g - base_q, slot).start()

        @pl.when(jnp.logical_and(g >= base_q + nq, g < base_q + nq + no))
        def _():
            o_copy(g - base_q - nq, slot).start()

    own_x = pltpu.make_async_copy(x_ref, xf.at[ds(core * sd, sd)], x_sem.at[2])
    own_x.start()
    rope_cp = pltpu.make_async_copy(rope_ref.at[:, ds(chip * ct, ct)], cs, x_sem.at[3])
    rope_cp.start()
    idx_cp = pltpu.make_async_copy(idx_ref, idx_v, x_sem.at[4])
    idx_cp.start()
    probs_cp = pltpu.make_async_copy(probs_ref, probs_v, x_sem.at[5])
    probs_cp.start()
    for i in range(nk):
        k_copy(i, 2 * i).start()
        v_copy(i, 2 * i + 1).start()

    barrier = pltpu.get_barrier_semaphore()

    @pl.loop(1, n)
    def _(off):
        pl.semaphore_signal(barrier, inc=1, device_id={"sp": lax.rem(me + off, n)}, device_id_type=MESH)

    pl.semaphore_wait(barrier, n - 1)

    def remote(src, dst, ssem, rsem, dev):
        return pltpu.make_async_remote_copy(src_ref=src, dst_ref=dst, send_sem=ssem, recv_sem=rsem,
                                            device_id={"sp": dev}, device_id_type=MESH)

    x_send = remote(x_ref, xf.at[ds(core * sd, sd)], x_sem.at[0], x_sem.at[1], partner)
    x_send.start()
    for i in range(nb - base_q):
        q_copy(i, base_q + i).start()

    ne = probs_ref.shape[0]
    top = idx_ref.shape[0]
    per = ne // n
    cap = 2 * sd * top // ne
    idx_cp.wait()
    probs_cp.wait()
    probs = probs_v[...]
    ei = lax.broadcasted_iota(jnp.int32, (ne, sd), 0)
    mine = jnp.zeros((ne, sd), F32)
    tot = None
    for c in range(top):
        hot = idx_v[c:c + 1, :] == ei
        mine = jnp.where(hot, 1.0, mine)
        sel = jnp.sum(jnp.where(hot, probs, 0.0), axis=0, keepdims=True)
        tot = sel if tot is None else tot + sel
    low = (lax.broadcasted_iota(jnp.int32, (sd, sd), 0) < lax.broadcasted_iota(jnp.int32, (sd, sd), 1))
    rank = jnp.dot(mine.astype(BF16), jnp.where(low, 1.0, 0.0).astype(BF16), preferred_element_type=F32)
    rank = jnp.where(mine > 0.5, rank, -1.0).T
    gate = (probs / tot).T
    rows = per * cap
    lane = lax.broadcasted_iota(jnp.int32, (sd, rows), 1)
    tok1 = (lax.broadcasted_iota(jnp.int32, (sd, rows), 0) + 1).astype(F32)
    sub = lax.broadcasted_iota(jnp.int32, (8, rows), 0)
    for d in range(n):
        rk = jnp.broadcast_to(rank[:, per * d:per * d + 1], (sd, rows))
        gt = jnp.broadcast_to(gate[:, per * d:per * d + 1], (sd, rows))
        for k in range(1, per):
            rk = jnp.where(lane >= k * cap, rank[:, per * d + k:per * d + k + 1], rk)
            gt = jnp.where(lane >= k * cap, gate[:, per * d + k:per * d + k + 1], gt)
        hit = rk == lax.rem(lane, cap).astype(F32)
        t_row = jnp.sum(jnp.where(hit, tok1, 0.0), axis=0, keepdims=True) - 1.0
        w_row = jnp.sum(jnp.where(hit, gt, 0.0), axis=0, keepdims=True)
        tw_own[d] = jnp.where(sub == 0, t_row, jnp.where(sub == 1, w_row, 0.0))
    tw_own_local = pltpu.make_async_copy(tw_own.at[me], tw_all.at[me], twr_sem.at[me])
    tw_own_local.start()

    def tw_send(off):
        d = lax.rem(me + off, n)
        return remote(tw_own.at[d], tw_all.at[me], tws_sem.at[d], twr_sem.at[me], d)

    @pl.loop(1, n)
    def _(off):
        tw_send(off).start()

    own_x.wait()
    rope_cp.wait()
    x_send.wait_recv()

    def rope(t):
        return t * cs[0] + pltpu.roll(t, HEAD // 2, 1) * cs[1]

    def kv_send(h, side):
        dev = right if side == 0 else left
        return remote(kvb.at[chip, h], kvb.at[chip, h], kvs_sem.at[side, h], kvr_sem.at[side, h], dev)

    def kv_forward(h):
        even = h % 2 == 0
        src = lchip if even else rchip
        dev = right if even else left
        return remote(kvb.at[src, h], kvb.at[src, h], kvf_sem.at[h], kvr_sem.at[2, h], dev)

    @pl.loop(0, nk)
    def _(i):
        k_copy(0, 2 * i).wait()
        v_copy(0, 2 * i + 1).wait()
        ka = jnp.dot(xf[...], wbuf[2 * i], preferred_element_type=F32)
        va = jnp.dot(xf[...], wbuf[2 * i + 1], preferred_element_type=F32)
        for hh in range(hpc):
            kvb[chip, hpc * i + hh, 0:ct] = rope(ka[:, hh * HEAD:(hh + 1) * HEAD]).astype(BF16)
        for hh in range(hpc):
            vt = va[:, hh * HEAD:(hh + 1) * HEAD].T.astype(BF16)
            for b in range(ct // HEAD):
                kvb[chip, hpc * i + hh, ct + b * HEAD:ct + (b + 1) * HEAD] = vt[:, b * HEAD:(b + 1) * HEAD]
        for hh in range(hpc):
            for side in range(2):
                kv_send(hpc * i + hh, side).start()
        fetch(2 * i + nb)
        fetch(2 * i + 1 + nb)

    def q_store(i):
        for hh in range(hpc):
            qt[i, :, hh * ct:(hh + 1) * ct] = rope(accs[:, hh * HEAD:(hh + 1) * HEAD]).T.astype(BF16)

    accs[...] = jnp.zeros_like(accs)
    fwd_at = [nq * 5 // 12 + (nq * 2 // 12) * h for h in range(heads_c)]

    @pl.loop(0, nq)
    def _(i):
        slot = lax.rem(base_q + i, nb)
        q_copy(0, slot).wait()
        q_store(jnp.maximum(i - 1, 0))
        accs[...] = jnp.dot(xf[...], wbuf[slot], preferred_element_type=F32)
        fetch(base_q + i + nb)
        for h in range(heads_c):
            @pl.when(i == fwd_at[h])
            def _(h=h):
                kv_send(h, h % 2).wait_recv()
                kv_forward(h).start()

    q_store(nq - 1)
    ex = math.log2(math.e) / math.sqrt(HEAD)
    wide = hpc * ct
    key_i = lax.broadcasted_iota(jnp.int32, (ct, wide), 0)
    qry_i = lax.rem(lax.broadcasted_iota(jnp.int32, (ct, wide), 1), ct)

    def attend(nc, h):
        cnt = m // hpc
        mx, inv = [None] * cnt, [None] * cnt

        def scores(g):
            q = qt[h * cnt + g]
            for j in range(nc):
                s = jnp.dot(kvb[j, h, 0:ct], q, preferred_element_type=F32)
                if j == nc - 1:
                    s = jnp.where(key_i <= qry_i, s, -jnp.inf)
                st[g, j] = s
                sm = jnp.max(s, axis=0, keepdims=True)
                mx[g] = sm if j == 0 else jnp.maximum(mx[g], sm)

        def soft(g):
            for j in range(nc):
                p = jnp.exp2((st[g, j] - mx[g]) * ex)
                st[g, j] = p
                ps = jnp.sum(p, axis=0, keepdims=True)
                tot = ps if j == 0 else tot + ps
            inv[g] = 1.0 / tot

        def out(g):
            for j in range(nc):
                vt = jnp.concatenate([kvb[j, h, ct + b * HEAD:ct + (b + 1) * HEAD] for b in range(ct // HEAD)], axis=1)
                oj = jnp.dot(vt, (st[g, j] * inv[g]).astype(BF16), preferred_element_type=F32)
                o = oj if j == 0 else o + oj
            o = jnp.concatenate([o[:, k * ct:(k + 1) * ct].T for k in range(hpc)], axis=1)
            of[core * heads_c + h, :, g * COL:(g + 1) * COL] = o.astype(BF16)

        for t in range(cnt + 2):
            if t >= 2:
                out(t - 2)
            if t < cnt:
                scores(t)
            if 1 <= t < cnt + 1:
                soft(t - 1)

    def o_send(h):
        return remote(of.at[core * heads_c + h], of.at[core * heads_c + h], os_sem.at[h], or_sem.at[h], partner)

    @pl.loop(0, heads_c)
    def _(h):
        even = lax.rem(h, 2) == 0
        @pl.when(even)
        def _():
            kv_send(h, 1).wait_recv()

        @pl.when(jnp.logical_not(even))
        def _():
            kv_send(h, 0).wait_recv()

        remote(kvb.at[fchip, h], kvb.at[fchip, h], kvf_sem.at[h], kvr_sem.at[2, h], right).wait_recv()
        for nc in range(1, chips + 1):
            @pl.when(chip == nc - 1)
            def _(nc=nc):
                attend(nc, h)
        o_send(h).start()

    @pl.loop(0, heads_c)
    def _(h):
        pltpu.make_async_copy(of.at[(1 - core) * heads_c + h], of.at[(1 - core) * heads_c + h], or_sem.at[h]).wait()

    def place(c, j, who):
        return hg_ref.at[c * no + j, ds(who * ct, ct)]

    def h_local(j):
        return pltpu.make_async_copy(ho.at[j], place(core, j, chip), hl_sem.at[j])

    def h_send(j, side):
        dev = (right, left, partner)[side]
        return remote(ho.at[j], place(core, j, chip), hs_sem.at[side, j],
                      hr_sem.at[side, j] if side < 2 else pr_sem.at[0, j], dev)

    def h_forward(j, side):
        src = (lchip, rchip)[side]
        dev = (right, left)[side]
        return remote(place(core, j, src), place(core, j, src), hf_sem.at[j], hr_sem.at[2, j], dev)

    def h_pass(j, k):
        src = (None, lchip, rchip, fchip)[k]
        return remote(place(core, j, src), place(core, j, src), hp_sem.at[k - 1, j], pr_sem.at[k, j], partner)

    group = m * HEAD

    @pl.loop(0, no)
    def _(j):
        slot = lax.rem(base_q + nq + j, nb)
        o_copy(0, slot).wait()
        acc = None
        for g in range(kvh):
            t = jnp.dot(of[g], wbuf[slot, g * group:(g + 1) * group], preferred_element_type=F32)
            acc = t if acc is None else acc + t
        xs = xf[:, ds(core * (no * COL) + j * COL, COL)].astype(F32)
        ho[j] = (xs + acc).astype(BF16)
        fetch(base_q + nq + j + nb)
        h_send(j, 0).start()
        h_send(j, 1).start()
        h_send(j, 2).start()
        h_local(j).start()

    tw_own_local.wait()

    @pl.loop(1, n)
    def _(off):
        d = lax.rem(me + off, n)
        pltpu.make_async_copy(tw_own.at[d], tw_all.at[d], twr_sem.at[d]).wait()

    li = lax.broadcasted_iota(jnp.int32, (rows, sd), 1).astype(F32)

    @pl.loop(0, n)
    def _(s):
        t = jnp.broadcast_to(tw_all[s, 0:1, :], (sd, rows)).T
        pick_ref[s] = jnp.where(t == li, 1.0, 0.0).astype(BF16)
        wcol_ref[s] = jnp.broadcast_to(tw_all[s, 1:2, :], (sd, rows)).T

    @pl.loop(0, no)
    def _(j):
        h_send(j, 0).wait_recv()
        even = lax.rem(j, 2) == 0

        @pl.when(even)
        def _():
            h_forward(j, 0).start()

        h_pass(j, 1).start()
        h_send(j, 1).wait_recv()

        @pl.when(jnp.logical_not(even))
        def _():
            h_forward(j, 1).start()

        h_pass(j, 2).start()

    @pl.loop(0, no)
    def _(j):
        h_forward(j, 0).wait_recv()
        h_pass(j, 3).start()

    @pl.loop(0, no)
    def _(j):
        for side in range(3):
            h_send(j, side).wait_send()
        h_local(j).wait()
        h_forward(j, 0).wait_send()
        for k in range(1, 4):
            h_pass(j, k).wait_send()
        for k in range(4):
            pltpu.make_async_copy(ho.at[j], place(core, j, chip), pr_sem.at[k, j]).wait()

    for h in range(heads_c):
        o_send(h).wait_send()
        kv_forward(h).wait_send()
        for side in range(2):
            kv_send(h, side).wait_send()
    x_send.wait_send()

    @pl.loop(1, n)
    def _(off):
        tw_send(off).wait_send()


def build_kernel(n, step, hg_ref, pick, wcol, h_ref, buf_ref, stage, h_sem, b_sem):
    nch, toks, col = hg_ref.shape
    sd = toks // n
    per = buf_ref.shape[0]
    rows = pick.shape[1]
    cap = rows // per
    me = lax.axis_index("sp")

    def ds(i, size):
        return pl.ds(pl.multiple_of(i, size), size)

    def h_copy(c):
        return pltpu.make_async_copy(hg_ref.at[c, ds(me * sd, sd)], h_ref.at[:, ds(c * col, col)], h_sem.at[c])

    def b_copy(i, slot):
        return pltpu.make_async_copy(stage.at[slot], buf_ref.at[:, :, ds(i * (step * col), step * col)], b_sem.at[slot])

    @pl.loop(0, nch)
    def _(c):
        h_copy(c).start()

    slots = stage.shape[0]

    @pl.loop(0, nch // step)
    def _(i):
        slot = lax.rem(i, slots)

        @pl.when(i >= slots)
        def _():
            b_copy(i, slot).wait()

        for k in range(step):
            for s in range(n):
                r = jnp.dot(pick[s], hg_ref[i * step + k, s * sd:(s + 1) * sd, :], preferred_element_type=F32)
                w = jnp.concatenate([wcol[s]] * (col // sd), axis=1)
                r = (w * r).astype(BF16)
                for e in range(per):
                    stage[slot, e, s * cap:(s + 1) * cap, k * col:(k + 1) * col] = r[e * cap:(e + 1) * cap]
        b_copy(i, slot).start()

    for k in range(slots):
        b_copy(0, k).wait()

    @pl.loop(0, nch)
    def _(c):
        h_copy(c).wait()


def solution(mesh):
    n = mesh.shape["sp"]
    row = P(("dp", "sp"), None)
    full = P(None, None)

    def local(x, wq, wk, wv, wo, idx, probs):
        sd, hid = x.shape
        heads = wq.shape[1] // HEAD
        kvh = wk.shape[1] // HEAD
        m = heads // kvh
        ne = probs.shape[1]
        per = ne // n
        cap = 2 * sd * idx.shape[1] // ne
        rows = per * cap
        chips = n // CORES
        ct = CORES * sd
        hc = kvh // CORES
        no = hid // CORES // COL
        nq = hc * m * HEAD // COL
        nb = 6
        dma = pltpu.SemaphoreType.DMA
        any_ = pl.BlockSpec(memory_space=pl.ANY)
        vm = pl.BlockSpec(memory_space=pltpu.VMEM)
        hg, pick, wcol = pl.pallas_call(
            functools.partial(block_kernel, n, kvh, m, nb),
            out_shape=(pltpu.VMEM((CORES * no, n * sd, COL), BF16),
                       pltpu.VMEM((n, rows, sd), BF16),
                       pltpu.VMEM((n, rows, sd), F32)),
            in_specs=[any_] * 8,
            out_specs=(any_, vm, vm),
            scratch_shapes=[
                pltpu.VMEM((ct, hid), BF16),
                pltpu.VMEM((nb, hid, COL), BF16),
                pltpu.VMEM((2, ct, HEAD), F32),
                pltpu.VMEM((chips, hc, 2 * ct, HEAD), BF16),
                pltpu.VMEM((nq, HEAD, COL // HEAD * ct), BF16),
                pltpu.VMEM((kvh, ct, m * HEAD), BF16),
                pltpu.VMEM((no, ct, COL), BF16),
                pltpu.VMEM((m * HEAD // COL, chips, ct, COL // HEAD * ct), F32),
                pltpu.VMEM((ct, COL), F32),
                pltpu.VMEM((n, 8, rows), F32),
                pltpu.VMEM((n, 8, rows), F32),
                pltpu.VMEM(idx.shape[::-1], jnp.int32),
                pltpu.VMEM(probs.shape[::-1], F32),
                dma((nb,)), dma((6,)), dma((n,)), dma((n,)),
                dma((2, hc)), dma((hc,)), dma((3, hc)), dma((hc,)), dma((hc,)),
                dma((no,)), dma((3, no)), dma((no,)), dma((3, no)), dma((3, no)), dma((4, no)),
            ],
            compiler_params=pltpu.CompilerParams(collective_id=0, has_side_effects=True,
                                                 vmem_limit_bytes=50_000_000),
        )(*(pltpu.with_memory_space_constraint(a, pltpu.HBM)
            for a in (x, wq, wk, wv, wo, idx.T, probs.T, jnp.asarray(rope_table(n * sd)))))

        step = 2
        h, buf = pl.pallas_call(
            functools.partial(build_kernel, n, step),
            out_shape=(jax.ShapeDtypeStruct((sd, hid), BF16),
                       jax.ShapeDtypeStruct((per, n * cap, hid), BF16)),
            in_specs=[vm, vm, vm],
            out_specs=(any_, any_),
            scratch_shapes=[pltpu.VMEM((3, per, n * cap, step * COL), BF16),
                            dma((CORES * no,)), dma((3,))],
            compiler_params=pltpu.CompilerParams(vmem_limit_bytes=30_000_000),
        )(hg, pick, wcol)
        return h, buf

    return jax.shard_map(local, mesh=mesh, in_specs=(row, full, full, full, full, row, row), out_specs=(row, P(("dp", "sp"), None, None)), check_vma=False)
```

```python
import functools
import math
import numpy as np
import jax
import jax.numpy as jnp
from jax import lax
from jax.experimental import pallas as pl
from jax.experimental.pallas import tpu as pltpu
from jax.sharding import PartitionSpec as P

HEAD = 128
ROPE_BASE = 1000000.0
CORES = 2
SHIFT = 1
COL = 256
F32 = jnp.float32
BF16 = jnp.bfloat16
MESH = pl.DeviceIdType.MESH


def rope_table(length):
    inv = ROPE_BASE ** (-np.arange(HEAD // 2, dtype=np.float64) * (2.0 / HEAD))
    ang = np.arange(length, dtype=np.float64)[:, None] * inv[None, :]
    c, s = np.cos(ang), np.sin(ang)
    return np.stack([np.concatenate([c, c], 1), np.concatenate([-s, s], 1)]).astype(np.float32)


def block_kernel(n, kvh, m, nb, x_ref, wq_ref, wk_ref, wv_ref, wo_ref, idx_ref, probs_ref, rope_ref,
                 hg_ref, pick_ref, wcol_ref,
                 xf, wbuf, cs, kvb, qt, of, ho, st, accs, tw_own, tw_all, idx_v, probs_v,
                 w_sem, x_sem, tws_sem, twr_sem, kvs_sem, kvf_sem, kvr_sem, os_sem, or_sem,
                 hl_sem, hs_sem, hf_sem, hp_sem, hr_sem, pr_sem):
    sd, hid = x_ref.shape
    chips = n // CORES
    ct = CORES * sd
    heads_c = kvh // CORES
    nk = heads_c * HEAD // COL
    nq = heads_c * m * HEAD // COL
    no = hid // CORES // COL
    hpc = COL // HEAD
    me = lax.axis_index("sp")
    chip = lax.div(me, CORES)
    core = lax.rem(me, CORES)
    partner = me + 1 - 2 * core
    right = lax.rem(me + CORES, n)
    left = lax.rem(me + n - CORES, n)
    rchip = lax.rem(chip + 1, chips)
    lchip = lax.rem(chip + chips - 1, chips)
    fchip = lax.rem(chip + 2, chips)

    def ds(i, size):
        return pl.ds(pl.multiple_of(i, size), size)

    def wcopy(src, col0, slot):
        return pltpu.make_async_copy(src.at[:, ds(col0, COL)], wbuf.at[slot], w_sem.at[slot])

    def k_copy(i, slot):
        return wcopy(wk_ref, core * (heads_c * HEAD) + i * COL, slot)

    def v_copy(i, slot):
        return wcopy(wv_ref, core * (heads_c * HEAD) + i * COL, slot)

    def q_copy(i, slot):
        return wcopy(wq_ref, core * (nq * COL) + i * COL, slot)

    def o_copy(i, slot):
        return wcopy(wo_ref, core * (no * COL) + i * COL, slot)

    base_q = 2 * nk

    def fetch(g):
        slot = lax.rem(g, nb)

        @pl.when(g < base_q + nq)
        def _():
            q_copy(g - base_q, slot).start()

        @pl.when(jnp.logical_and(g >= base_q + nq, g < base_q + nq + no))
        def _():
            o_copy(g - base_q - nq, slot).start()

    own_x = pltpu.make_async_copy(x_ref, xf.at[ds(core * sd, sd)], x_sem.at[2])
    own_x.start()
    rope_cp = pltpu.make_async_copy(rope_ref.at[:, ds(chip * ct, ct)], cs, x_sem.at[3])
    rope_cp.start()
    idx_cp = pltpu.make_async_copy(idx_ref, idx_v, x_sem.at[4])
    idx_cp.start()
    probs_cp = pltpu.make_async_copy(probs_ref, probs_v, x_sem.at[5])
    probs_cp.start()
    for i in range(nk):
        k_copy(i, 2 * i).start()
        v_copy(i, 2 * i + 1).start()

    barrier = pltpu.get_barrier_semaphore()

    @pl.loop(1, n)
    def _(off):
        pl.semaphore_signal(barrier, inc=1, device_id={"sp": lax.rem(me + off, n)}, device_id_type=MESH)

    pl.semaphore_wait(barrier, n - 1)

    def remote(src, dst, ssem, rsem, dev):
        return pltpu.make_async_remote_copy(src_ref=src, dst_ref=dst, send_sem=ssem, recv_sem=rsem,
                                            device_id={"sp": dev}, device_id_type=MESH)

    x_send = remote(x_ref, xf.at[ds(core * sd, sd)], x_sem.at[0], x_sem.at[1], partner)
    x_send.start()
    for i in range(nb - base_q):
        q_copy(i, base_q + i).start()

    ne = probs_ref.shape[0]
    top = idx_ref.shape[0]
    per = ne // n
    cap = 2 * sd * top // ne
    idx_cp.wait()
    probs_cp.wait()
    probs = probs_v[...]
    ei = lax.broadcasted_iota(jnp.int32, (ne, sd), 0)
    mine = jnp.zeros((ne, sd), F32)
    tot = None
    for c in range(top):
        hot = idx_v[c:c + 1, :] == ei
        mine = jnp.where(hot, 1.0, mine)
        sel = jnp.sum(jnp.where(hot, probs, 0.0), axis=0, keepdims=True)
        tot = sel if tot is None else tot + sel
    low = (lax.broadcasted_iota(jnp.int32, (sd, sd), 0) < lax.broadcasted_iota(jnp.int32, (sd, sd), 1))
    rank = jnp.dot(mine.astype(BF16), jnp.where(low, 1.0, 0.0).astype(BF16), preferred_element_type=F32)
    rank = jnp.where(mine > 0.5, rank, -1.0).T
    gate = (probs / tot).T
    rows = per * cap
    lane = lax.broadcasted_iota(jnp.int32, (sd, rows), 1)
    tok1 = (lax.broadcasted_iota(jnp.int32, (sd, rows), 0) + 1).astype(F32)
    sub = lax.broadcasted_iota(jnp.int32, (8, rows), 0)
    for d in range(n):
        rk = jnp.broadcast_to(rank[:, per * d:per * d + 1], (sd, rows))
        gt = jnp.broadcast_to(gate[:, per * d:per * d + 1], (sd, rows))
        for k in range(1, per):
            rk = jnp.where(lane >= k * cap, rank[:, per * d + k:per * d + k + 1], rk)
            gt = jnp.where(lane >= k * cap, gate[:, per * d + k:per * d + k + 1], gt)
        hit = rk == lax.rem(lane, cap).astype(F32)
        t_row = jnp.sum(jnp.where(hit, tok1, 0.0), axis=0, keepdims=True) - 1.0
        w_row = jnp.sum(jnp.where(hit, gt, 0.0), axis=0, keepdims=True)
        tw_own[d] = jnp.where(sub == 0, t_row, jnp.where(sub == 1, w_row, 0.0))
    tw_own_local = pltpu.make_async_copy(tw_own.at[me], tw_all.at[me], twr_sem.at[me])
    tw_own_local.start()

    def tw_send(off):
        d = lax.rem(me + off, n)
        return remote(tw_own.at[d], tw_all.at[me], tws_sem.at[d], twr_sem.at[me], d)

    @pl.loop(1, n)
    def _(off):
        tw_send(off).start()

    own_x.wait()
    rope_cp.wait()
    x_send.wait_recv()

    def rope(t):
        return t * cs[0] + pltpu.roll(t, HEAD // 2, 1) * cs[1]

    def kv_send(h, side):
        dev = right if side == 0 else left
        return remote(kvb.at[chip, h], kvb.at[chip, h], kvs_sem.at[side, h], kvr_sem.at[side, h], dev)

    def kv_forward(h):
        even = h % 2 == 0
        src = lchip if even else rchip
        dev = right if even else left
        return remote(kvb.at[src, h], kvb.at[src, h], kvf_sem.at[h], kvr_sem.at[2, h], dev)

    @pl.loop(0, nk)
    def _(i):
        k_copy(0, 2 * i).wait()
        v_copy(0, 2 * i + 1).wait()
        ka = jnp.dot(xf[...], wbuf[2 * i], preferred_element_type=F32)
        va = jnp.dot(xf[...], wbuf[2 * i + 1], preferred_element_type=F32)
        for hh in range(hpc):
            kvb[chip, hpc * i + hh, 0:ct] = rope(ka[:, hh * HEAD:(hh + 1) * HEAD]).astype(BF16)
        for hh in range(hpc):
            vt = va[:, hh * HEAD:(hh + 1) * HEAD].T.astype(BF16)
            for b in range(ct // HEAD):
                kvb[chip, hpc * i + hh, ct + b * HEAD:ct + (b + 1) * HEAD] = vt[:, b * HEAD:(b + 1) * HEAD]
        for hh in range(hpc):
            for side in range(2):
                kv_send(hpc * i + hh, side).start()
        fetch(2 * i + nb)
        fetch(2 * i + 1 + nb)

    def q_store(i):
        for hh in range(hpc):
            qt[i, :, hh * ct:(hh + 1) * ct] = rope(accs[:, hh * HEAD:(hh + 1) * HEAD]).T.astype(BF16)

    accs[...] = jnp.zeros_like(accs)
    fwd_at = [nq * 5 // 12 + (nq * 2 // 12) * h for h in range(heads_c)]

    @pl.loop(0, nq)
    def _(i):
        slot = lax.rem(base_q + i, nb)
        q_copy(0, slot).wait()
        q_store(jnp.maximum(i - 1, 0))
        accs[...] = jnp.dot(xf[...], wbuf[slot], preferred_element_type=F32)
        fetch(base_q + i + nb)
        for h in range(heads_c):
            @pl.when(i == fwd_at[h])
            def _(h=h):
                kv_send(h, h % 2).wait_recv()
                kv_forward(h).start()

    q_store(nq - 1)
    ex = math.log2(math.e) / math.sqrt(HEAD)
    wide = hpc * ct
    key_i = lax.broadcasted_iota(jnp.int32, (ct, wide), 0)
    qry_i = lax.rem(lax.broadcasted_iota(jnp.int32, (ct, wide), 1), ct)

    def attend(nc, h):
        cnt = m // hpc
        mx, inv = [None] * cnt, [None] * cnt

        def scores(g):
            q = qt[h * cnt + g]
            for j in range(nc):
                s = jnp.dot(kvb[j, h, 0:ct], q, preferred_element_type=F32)
                if j == nc - 1:
                    s = jnp.where(key_i <= qry_i, s, -jnp.inf)
                st[g, j] = s
                sm = jnp.max(s, axis=0, keepdims=True)
                mx[g] = sm if j == 0 else jnp.maximum(mx[g], sm)

        def soft(g):
            for j in range(nc):
                p = jnp.exp2((st[g, j] - mx[g]) * ex)
                st[g, j] = p
                ps = jnp.sum(p, axis=0, keepdims=True)
                tot = ps if j == 0 else tot + ps
            inv[g] = 1.0 / tot

        def out(g):
            for j in range(nc):
                vt = jnp.concatenate([kvb[j, h, ct + b * HEAD:ct + (b + 1) * HEAD] for b in range(ct // HEAD)], axis=1)
                oj = jnp.dot(vt, (st[g, j] * inv[g]).astype(BF16), preferred_element_type=F32)
                o = oj if j == 0 else o + oj
            o = jnp.concatenate([o[:, k * ct:(k + 1) * ct].T for k in range(hpc)], axis=1)
            of[core * heads_c + h, :, g * COL:(g + 1) * COL] = o.astype(BF16)

        for t in range(cnt + 2):
            if t >= 2:
                out(t - 2)
            if t < cnt:
                scores(t)
            if 1 <= t < cnt + 1:
                soft(t - 1)

    def o_send(h):
        return remote(of.at[core * heads_c + h], of.at[core * heads_c + h], os_sem.at[h], or_sem.at[h], partner)

    @pl.loop(0, heads_c)
    def _(h):
        even = lax.rem(h, 2) == 0
        @pl.when(even)
        def _():
            kv_send(h, 1).wait_recv()

        @pl.when(jnp.logical_not(even))
        def _():
            kv_send(h, 0).wait_recv()

        remote(kvb.at[fchip, h], kvb.at[fchip, h], kvf_sem.at[h], kvr_sem.at[2, h], right).wait_recv()
        for nc in range(1, chips + 1):
            @pl.when(chip == nc - 1)
            def _(nc=nc):
                attend(nc, h)
        o_send(h).start()

    @pl.loop(0, heads_c)
    def _(h):
        pltpu.make_async_copy(of.at[(1 - core) * heads_c + h], of.at[(1 - core) * heads_c + h], or_sem.at[h]).wait()

    def place(c, j, who):
        return hg_ref.at[c * no + j, ds(who * ct, ct)]

    def h_local(j):
        return pltpu.make_async_copy(ho.at[j], place(core, j, chip), hl_sem.at[j])

    def h_send(j, side):
        dev = (right, left, partner)[side]
        return remote(ho.at[j], place(core, j, chip), hs_sem.at[side, j],
                      hr_sem.at[side, j] if side < 2 else pr_sem.at[0, j], dev)

    def h_forward(j, side):
        src = (lchip, rchip)[side]
        dev = (right, left)[side]
        return remote(place(core, j, src), place(core, j, src), hf_sem.at[side, j], hr_sem.at[2, j], dev)

    def h_pass(j, k):
        src = (None, lchip, rchip, fchip)[k]
        return remote(place(core, j, src), place(core, j, src), hp_sem.at[k - 1, j], pr_sem.at[k, j], partner)

    group = m * HEAD

    last = chip == chips - 1
    across = chip == lax.rem(chips + 1, chips)

    def sends_on(j, side):
        kind = lax.rem(j, 2) == side
        late = j >= no - 2 * SHIFT
        return jnp.logical_or(jnp.logical_and(kind, jnp.logical_not(jnp.logical_and(late, last))),
                              jnp.logical_and(late, across))

    @pl.loop(0, no)
    def _(j):
        slot = lax.rem(base_q + nq + j, nb)
        o_copy(0, slot).wait()
        acc = None
        for g in range(kvh):
            t = jnp.dot(of[g], wbuf[slot, g * group:(g + 1) * group], preferred_element_type=F32)
            acc = t if acc is None else acc + t
        xs = xf[:, ds(core * (no * COL) + j * COL, COL)].astype(F32)
        ho[j] = (xs + acc).astype(BF16)
        fetch(base_q + nq + j + nb)
        h_send(j, 0).start()
        h_send(j, 1).start()
        h_send(j, 2).start()
        h_local(j).start()

    tw_own_local.wait()

    @pl.loop(1, n)
    def _(off):
        d = lax.rem(me + off, n)
        pltpu.make_async_copy(tw_own.at[d], tw_all.at[d], twr_sem.at[d]).wait()

    li = lax.broadcasted_iota(jnp.int32, (rows, sd), 1).astype(F32)

    @pl.loop(0, n)
    def _(s):
        t = jnp.broadcast_to(tw_all[s, 0:1, :], (sd, rows)).T
        pick_ref[s] = jnp.where(t == li, 1.0, 0.0).astype(BF16)
        wcol_ref[s] = jnp.broadcast_to(tw_all[s, 1:2, :], (sd, rows)).T

    @pl.loop(0, no)
    def _(j):
        h_send(j, 0).wait_recv()

        @pl.when(sends_on(j, 0))
        def _():
            h_forward(j, 0).start()

        h_pass(j, 1).start()
        h_send(j, 1).wait_recv()

        @pl.when(sends_on(j, 1))
        def _():
            h_forward(j, 1).start()

        h_pass(j, 2).start()

    @pl.loop(0, no)
    def _(j):
        h_forward(j, 0).wait_recv()
        h_pass(j, 3).start()

    @pl.loop(0, no)
    def _(j):
        for side in range(3):
            h_send(j, side).wait_send()
        h_local(j).wait()
        for side in range(2):
            @pl.when(sends_on(j, side))
            def _(side=side):
                h_forward(j, side).wait_send()
        for k in range(1, 4):
            h_pass(j, k).wait_send()
        for k in range(4):
            pltpu.make_async_copy(ho.at[j], place(core, j, chip), pr_sem.at[k, j]).wait()

    for h in range(heads_c):
        o_send(h).wait_send()
        kv_forward(h).wait_send()
        for side in range(2):
            kv_send(h, side).wait_send()
    x_send.wait_send()

    @pl.loop(1, n)
    def _(off):
        tw_send(off).wait_send()


def build_kernel(n, step, hg_ref, pick, wcol, h_ref, buf_ref, stage, h_sem, b_sem):
    nch, toks, col = hg_ref.shape
    sd = toks // n
    per = buf_ref.shape[0]
    rows = pick.shape[1]
    cap = rows // per
    me = lax.axis_index("sp")

    def ds(i, size):
        return pl.ds(pl.multiple_of(i, size), size)

    def h_copy(c):
        return pltpu.make_async_copy(hg_ref.at[c, ds(me * sd, sd)], h_ref.at[:, ds(c * col, col)], h_sem.at[c])

    def b_copy(i, slot):
        return pltpu.make_async_copy(stage.at[slot], buf_ref.at[:, :, ds(i * (step * col), step * col)], b_sem.at[slot])

    @pl.loop(0, nch)
    def _(c):
        h_copy(c).start()

    slots = stage.shape[0]

    @pl.loop(0, nch // step)
    def _(i):
        slot = lax.rem(i, slots)

        @pl.when(i >= slots)
        def _():
            b_copy(i, slot).wait()

        for k in range(step):
            for s in range(n):
                r = jnp.dot(pick[s], hg_ref[i * step + k, s * sd:(s + 1) * sd, :], preferred_element_type=F32)
                w = jnp.concatenate([wcol[s]] * (col // sd), axis=1)
                r = (w * r).astype(BF16)
                for e in range(per):
                    stage[slot, e, s * cap:(s + 1) * cap, k * col:(k + 1) * col] = r[e * cap:(e + 1) * cap]
        b_copy(i, slot).start()

    for k in range(slots):
        b_copy(0, k).wait()

    @pl.loop(0, nch)
    def _(c):
        h_copy(c).wait()


def solution(mesh):
    n = mesh.shape["sp"]
    row = P(("dp", "sp"), None)
    full = P(None, None)

    def local(x, wq, wk, wv, wo, idx, probs):
        sd, hid = x.shape
        heads = wq.shape[1] // HEAD
        kvh = wk.shape[1] // HEAD
        m = heads // kvh
        ne = probs.shape[1]
        per = ne // n
        cap = 2 * sd * idx.shape[1] // ne
        rows = per * cap
        chips = n // CORES
        ct = CORES * sd
        hc = kvh // CORES
        no = hid // CORES // COL
        nq = hc * m * HEAD // COL
        nb = 6
        dma = pltpu.SemaphoreType.DMA
        any_ = pl.BlockSpec(memory_space=pl.ANY)
        vm = pl.BlockSpec(memory_space=pltpu.VMEM)
        hg, pick, wcol = pl.pallas_call(
            functools.partial(block_kernel, n, kvh, m, nb),
            out_shape=(pltpu.VMEM((CORES * no, n * sd, COL), BF16),
                       pltpu.VMEM((n, rows, sd), BF16),
                       pltpu.VMEM((n, rows, sd), F32)),
            in_specs=[any_] * 8,
            out_specs=(any_, vm, vm),
            scratch_shapes=[
                pltpu.VMEM((ct, hid), BF16),
                pltpu.VMEM((nb, hid, COL), BF16),
                pltpu.VMEM((2, ct, HEAD), F32),
                pltpu.VMEM((chips, hc, 2 * ct, HEAD), BF16),
                pltpu.VMEM((nq, HEAD, COL // HEAD * ct), BF16),
                pltpu.VMEM((kvh, ct, m * HEAD), BF16),
                pltpu.VMEM((no, ct, COL), BF16),
                pltpu.VMEM((m * HEAD // COL, chips, ct, COL // HEAD * ct), F32),
                pltpu.VMEM((ct, COL), F32),
                pltpu.VMEM((n, 8, rows), F32),
                pltpu.VMEM((n, 8, rows), F32),
                pltpu.VMEM(idx.shape[::-1], jnp.int32),
                pltpu.VMEM(probs.shape[::-1], F32),
                dma((nb,)), dma((6,)), dma((n,)), dma((n,)),
                dma((2, hc)), dma((hc,)), dma((3, hc)), dma((hc,)), dma((hc,)),
                dma((no,)), dma((3, no)), dma((2, no)), dma((3, no)), dma((3, no)), dma((4, no)),
            ],
            compiler_params=pltpu.CompilerParams(collective_id=0, has_side_effects=True,
                                                 vmem_limit_bytes=50_000_000),
        )(*(pltpu.with_memory_space_constraint(a, pltpu.HBM)
            for a in (x, wq, wk, wv, wo, idx.T, probs.T, jnp.asarray(rope_table(n * sd)))))

        step = 2
        h, buf = pl.pallas_call(
            functools.partial(build_kernel, n, step),
            out_shape=(jax.ShapeDtypeStruct((sd, hid), BF16),
                       jax.ShapeDtypeStruct((per, n * cap, hid), BF16)),
            in_specs=[vm, vm, vm],
            out_specs=(any_, any_),
            scratch_shapes=[pltpu.VMEM((3, per, n * cap, step * COL), BF16),
                            dma((CORES * no,)), dma((3,))],
            compiler_params=pltpu.CompilerParams(vmem_limit_bytes=30_000_000),
        )(hg, pick, wcol)
        return h, buf

    return jax.shard_map(local, mesh=mesh, in_specs=(row, full, full, full, full, row, row), out_specs=(row, P(("dp", "sp"), None, None)), check_vma=False)
```

```python
import functools
import math
import numpy as np
import jax
import jax.numpy as jnp
from jax import lax
from jax.experimental import pallas as pl
from jax.experimental.pallas import tpu as pltpu
from jax.sharding import PartitionSpec as P

HEAD = 128
ROPE_BASE = 1000000.0
CORES = 2
SHIFT = 1
COL = 256
F32 = jnp.float32
BF16 = jnp.bfloat16
MESH = pl.DeviceIdType.MESH


def rope_table(length):
    inv = ROPE_BASE ** (-np.arange(HEAD // 2, dtype=np.float64) * (2.0 / HEAD))
    ang = np.arange(length, dtype=np.float64)[:, None] * inv[None, :]
    c, s = np.cos(ang), np.sin(ang)
    return np.stack([np.concatenate([c, c], 1), np.concatenate([-s, s], 1)]).astype(np.float32)


def block_kernel(n, kvh, m, nb, x_ref, wq_ref, wk_ref, wv_ref, wo_ref, idx_ref, probs_ref, rope_ref,
                 hg_ref, pick_ref, wcol_ref,
                 xf, wbuf, cs, kvb, qt, of, ho, st, accs, tw_own, tw_all, idx_v, probs_v,
                 w_sem, x_sem, tws_sem, twr_sem, kvs_sem, kvf_sem, kvr_sem, os_sem, or_sem,
                 hl_sem, hs_sem, hf_sem, hp_sem, hr_sem, pr_sem):
    sd, hid = x_ref.shape
    chips = n // CORES
    ct = CORES * sd
    heads_c = kvh // CORES
    nk = heads_c * HEAD // COL
    nq = heads_c * m * HEAD // COL
    no = hid // CORES // COL
    hpc = COL // HEAD
    me = lax.axis_index("sp")
    chip = lax.div(me, CORES)
    core = lax.rem(me, CORES)
    partner = me + 1 - 2 * core
    right = lax.rem(me + CORES, n)
    left = lax.rem(me + n - CORES, n)
    rchip = lax.rem(chip + 1, chips)
    lchip = lax.rem(chip + chips - 1, chips)
    fchip = lax.rem(chip + 2, chips)

    def ds(i, size):
        return pl.ds(pl.multiple_of(i, size), size)

    def wcopy(src, col0, slot):
        return pltpu.make_async_copy(src.at[:, ds(col0, COL)], wbuf.at[slot], w_sem.at[slot])

    def k_copy(i, slot):
        return wcopy(wk_ref, core * (heads_c * HEAD) + i * COL, slot)

    def v_copy(i, slot):
        return wcopy(wv_ref, core * (heads_c * HEAD) + i * COL, slot)

    def q_copy(i, slot):
        return wcopy(wq_ref, core * (nq * COL) + i * COL, slot)

    def o_copy(i, slot):
        return wcopy(wo_ref, core * (no * COL) + i * COL, slot)

    base_q = 2 * nk

    def fetch(g):
        slot = lax.rem(g, nb)

        @pl.when(g < base_q + nq)
        def _():
            q_copy(g - base_q, slot).start()

        @pl.when(jnp.logical_and(g >= base_q + nq, g < base_q + nq + no))
        def _():
            o_copy(g - base_q - nq, slot).start()

    own_x = pltpu.make_async_copy(x_ref, xf.at[ds(core * sd, sd)], x_sem.at[2])
    own_x.start()
    rope_cp = pltpu.make_async_copy(rope_ref.at[:, ds(chip * ct, ct)], cs, x_sem.at[3])
    rope_cp.start()
    idx_cp = pltpu.make_async_copy(idx_ref, idx_v, x_sem.at[4])
    idx_cp.start()
    probs_cp = pltpu.make_async_copy(probs_ref, probs_v, x_sem.at[5])
    probs_cp.start()
    for i in range(nk):
        k_copy(i, 2 * i).start()
        v_copy(i, 2 * i + 1).start()

    barrier = pltpu.get_barrier_semaphore()

    @pl.loop(1, n)
    def _(off):
        pl.semaphore_signal(barrier, inc=1, device_id={"sp": lax.rem(me + off, n)}, device_id_type=MESH)

    pl.semaphore_wait(barrier, n - 1)

    def remote(src, dst, ssem, rsem, dev):
        return pltpu.make_async_remote_copy(src_ref=src, dst_ref=dst, send_sem=ssem, recv_sem=rsem,
                                            device_id={"sp": dev}, device_id_type=MESH)

    x_send = remote(x_ref, xf.at[ds(core * sd, sd)], x_sem.at[0], x_sem.at[1], partner)
    x_send.start()
    for i in range(nb - base_q):
        q_copy(i, base_q + i).start()

    ne = probs_ref.shape[0]
    top = idx_ref.shape[0]
    per = ne // n
    cap = 2 * sd * top // ne
    idx_cp.wait()
    probs_cp.wait()
    probs = probs_v[...]
    ei = lax.broadcasted_iota(jnp.int32, (ne, sd), 0)
    mine = jnp.zeros((ne, sd), F32)
    tot = None
    for c in range(top):
        hot = idx_v[c:c + 1, :] == ei
        mine = jnp.where(hot, 1.0, mine)
        sel = jnp.sum(jnp.where(hot, probs, 0.0), axis=0, keepdims=True)
        tot = sel if tot is None else tot + sel
    low = (lax.broadcasted_iota(jnp.int32, (sd, sd), 0) < lax.broadcasted_iota(jnp.int32, (sd, sd), 1))
    rank = jnp.dot(mine.astype(BF16), jnp.where(low, 1.0, 0.0).astype(BF16), preferred_element_type=F32)
    rank = jnp.where(mine > 0.5, rank, -1.0).T
    gate = (probs / tot).T
    rows = per * cap
    lane = lax.broadcasted_iota(jnp.int32, (sd, rows), 1)
    tok1 = (lax.broadcasted_iota(jnp.int32, (sd, rows), 0) + 1).astype(F32)
    sub = lax.broadcasted_iota(jnp.int32, (8, rows), 0)
    for d in range(n):
        rk = jnp.broadcast_to(rank[:, per * d:per * d + 1], (sd, rows))
        gt = jnp.broadcast_to(gate[:, per * d:per * d + 1], (sd, rows))
        for k in range(1, per):
            rk = jnp.where(lane >= k * cap, rank[:, per * d + k:per * d + k + 1], rk)
            gt = jnp.where(lane >= k * cap, gate[:, per * d + k:per * d + k + 1], gt)
        hit = rk == lax.rem(lane, cap).astype(F32)
        t_row = jnp.sum(jnp.where(hit, tok1, 0.0), axis=0, keepdims=True) - 1.0
        w_row = jnp.sum(jnp.where(hit, gt, 0.0), axis=0, keepdims=True)
        tw_own[d] = jnp.where(sub == 0, t_row, jnp.where(sub == 1, w_row, 0.0))
    tw_own_local = pltpu.make_async_copy(tw_own.at[me], tw_all.at[me], twr_sem.at[me])
    tw_own_local.start()

    def tw_send(off):
        d = lax.rem(me + off, n)
        return remote(tw_own.at[d], tw_all.at[me], tws_sem.at[d], twr_sem.at[me], d)

    @pl.loop(1, n)
    def _(off):
        tw_send(off).start()

    own_x.wait()
    rope_cp.wait()
    x_send.wait_recv()

    def rope(t):
        return t * cs[0] + pltpu.roll(t, HEAD // 2, 1) * cs[1]

    def kv_send(h, side):
        dev = right if side == 0 else left
        return remote(kvb.at[chip, h], kvb.at[chip, h], kvs_sem.at[side, h], kvr_sem.at[side, h], dev)

    def kv_forward(h):
        even = h % 2 == 0
        src = lchip if even else rchip
        dev = right if even else left
        return remote(kvb.at[src, h], kvb.at[src, h], kvf_sem.at[h], kvr_sem.at[2, h], dev)

    @pl.loop(0, nk)
    def _(i):
        k_copy(0, 2 * i).wait()
        v_copy(0, 2 * i + 1).wait()
        ka = jnp.dot(xf[...], wbuf[2 * i], preferred_element_type=F32)
        va = jnp.dot(xf[...], wbuf[2 * i + 1], preferred_element_type=F32)
        for hh in range(hpc):
            kvb[chip, hpc * i + hh, 0:ct] = rope(ka[:, hh * HEAD:(hh + 1) * HEAD]).astype(BF16)
        for hh in range(hpc):
            vt = va[:, hh * HEAD:(hh + 1) * HEAD].T.astype(BF16)
            for b in range(ct // HEAD):
                kvb[chip, hpc * i + hh, ct + b * HEAD:ct + (b + 1) * HEAD] = vt[:, b * HEAD:(b + 1) * HEAD]
        for hh in range(hpc):
            for side in range(2):
                kv_send(hpc * i + hh, side).start()
        fetch(2 * i + nb)
        fetch(2 * i + 1 + nb)

    def q_store(i):
        for hh in range(hpc):
            qt[i, :, hh * ct:(hh + 1) * ct] = rope(accs[:, hh * HEAD:(hh + 1) * HEAD]).T.astype(BF16)

    accs[...] = jnp.zeros_like(accs)
    fwd_at = [nq * 5 // 12 + (nq * 2 // 12) * h for h in range(heads_c)]

    @pl.loop(0, nq)
    def _(i):
        slot = lax.rem(base_q + i, nb)
        q_copy(0, slot).wait()
        q_store(jnp.maximum(i - 1, 0))
        accs[...] = jnp.dot(xf[...], wbuf[slot], preferred_element_type=F32)
        fetch(base_q + i + nb)
        for h in range(heads_c):
            @pl.when(i == fwd_at[h])
            def _(h=h):
                kv_send(h, h % 2).wait_recv()
                kv_forward(h).start()

    q_store(nq - 1)
    ex = math.log2(math.e) / math.sqrt(HEAD)
    wide = hpc * ct
    key_i = lax.broadcasted_iota(jnp.int32, (ct, wide), 0)
    qry_i = lax.rem(lax.broadcasted_iota(jnp.int32, (ct, wide), 1), ct)

    def attend(nc, h):
        cnt = m // hpc
        mx, inv = [None] * cnt, [None] * cnt

        def scores(g):
            q = qt[h * cnt + g]
            for j in range(nc):
                s = jnp.dot(kvb[j, h, 0:ct], q, preferred_element_type=F32)
                if j == nc - 1:
                    s = jnp.where(key_i <= qry_i, s, -jnp.inf)
                st[g, j] = s
                sm = jnp.max(s, axis=0, keepdims=True)
                mx[g] = sm if j == 0 else jnp.maximum(mx[g], sm)

        def soft(g):
            for j in range(nc):
                p = jnp.exp2((st[g, j] - mx[g]) * ex)
                st[g, j] = p
                ps = jnp.sum(p, axis=0, keepdims=True)
                tot = ps if j == 0 else tot + ps
            inv[g] = 1.0 / tot

        def out(g):
            for j in range(nc):
                vt = jnp.concatenate([kvb[j, h, ct + b * HEAD:ct + (b + 1) * HEAD] for b in range(ct // HEAD)], axis=1)
                oj = jnp.dot(vt, (st[g, j] * inv[g]).astype(BF16), preferred_element_type=F32)
                o = oj if j == 0 else o + oj
            o = jnp.concatenate([o[:, k * ct:(k + 1) * ct].T for k in range(hpc)], axis=1)
            of[core * heads_c + h, :, g * COL:(g + 1) * COL] = o.astype(BF16)

        for t in range(cnt + 2):
            if t >= 2:
                out(t - 2)
            if t < cnt:
                scores(t)
            if 1 <= t < cnt + 1:
                soft(t - 1)

    def o_send(h):
        return remote(of.at[core * heads_c + h], of.at[core * heads_c + h], os_sem.at[h], or_sem.at[h], partner)

    @pl.loop(0, heads_c)
    def _(h):
        even = lax.rem(h, 2) == 0
        @pl.when(even)
        def _():
            kv_send(h, 1).wait_recv()

        @pl.when(jnp.logical_not(even))
        def _():
            kv_send(h, 0).wait_recv()

        remote(kvb.at[fchip, h], kvb.at[fchip, h], kvf_sem.at[h], kvr_sem.at[2, h], right).wait_recv()
        for nc in range(1, chips + 1):
            @pl.when(chip == nc - 1)
            def _(nc=nc):
                attend(nc, h)
        o_send(h).start()

    @pl.loop(0, heads_c)
    def _(h):
        pltpu.make_async_copy(of.at[(1 - core) * heads_c + h], of.at[(1 - core) * heads_c + h], or_sem.at[h]).wait()

    def place(c, j, who):
        return hg_ref.at[c * no + j, ds(who * ct, ct)]

    def h_local(j):
        return pltpu.make_async_copy(ho.at[j], place(core, j, chip), hl_sem.at[j])

    def h_send(j, side):
        dev = (right, left, partner)[side]
        return remote(ho.at[j], place(core, j, chip), hs_sem.at[side, j],
                      hr_sem.at[side, j] if side < 2 else pr_sem.at[0, j], dev)

    def h_forward(j, side):
        src = (lchip, rchip)[side]
        dev = (right, left)[side]
        return remote(place(core, j, src), place(core, j, src), hf_sem.at[side, j], hr_sem.at[2, j], dev)

    def h_pass(j, k):
        src = (None, lchip, rchip, fchip)[k]
        return remote(place(core, j, src), place(core, j, src), hp_sem.at[k - 1, j], pr_sem.at[k, j], partner)

    group = m * HEAD

    last = chip == chips - 1
    across = chip == lax.rem(chips + 1, chips)

    def sends_on(j, side):
        kind = lax.rem(j, 2) == side
        late = j >= no - 2 * SHIFT
        return jnp.logical_or(jnp.logical_and(kind, jnp.logical_not(jnp.logical_and(late, last))),
                              jnp.logical_and(late, across))

    @pl.loop(0, no)
    def _(j):
        slot = lax.rem(base_q + nq + j, nb)
        o_copy(0, slot).wait()
        acc = None
        for g in range(kvh):
            t = jnp.dot(of[g], wbuf[slot, g * group:(g + 1) * group], preferred_element_type=F32)
            acc = t if acc is None else acc + t
        xs = xf[:, ds(core * (no * COL) + j * COL, COL)].astype(F32)
        ho[j] = (xs + acc).astype(BF16)
        fetch(base_q + nq + j + nb)
        h_send(j, 0).start()
        h_send(j, 1).start()
        h_send(j, 2).start()
        h_local(j).start()

    tw_own_local.wait()

    @pl.loop(1, n)
    def _(off):
        d = lax.rem(me + off, n)
        pltpu.make_async_copy(tw_own.at[d], tw_all.at[d], twr_sem.at[d]).wait()

    li = lax.broadcasted_iota(jnp.int32, (rows, sd), 1).astype(F32)

    @pl.loop(0, n)
    def _(s):
        t = jnp.broadcast_to(tw_all[s, 0:1, :], (sd, rows)).T
        pick_ref[s] = jnp.where(t == li, 1.0, 0.0).astype(BF16)
        wcol_ref[s] = jnp.broadcast_to(tw_all[s, 1:2, :], (sd, rows)).T

    @pl.loop(0, no)
    def _(j):
        h_send(j, 0).wait_recv()

        @pl.when(sends_on(j, 0))
        def _():
            h_forward(j, 0).start()

        h_pass(j, 1).start()
        h_send(j, 1).wait_recv()

        @pl.when(sends_on(j, 1))
        def _():
            h_forward(j, 1).start()

        h_pass(j, 2).start()

    @pl.loop(0, no)
    def _(j):
        h_forward(j, 0).wait_recv()
        h_pass(j, 3).start()

    @pl.loop(0, no)
    def _(j):
        for side in range(3):
            h_send(j, side).wait_send()
        h_local(j).wait()
        for side in range(2):
            @pl.when(sends_on(j, side))
            def _(side=side):
                h_forward(j, side).wait_send()
        for k in range(1, 4):
            h_pass(j, k).wait_send()
        for k in range(4):
            pltpu.make_async_copy(ho.at[j], place(core, j, chip), pr_sem.at[k, j]).wait()

    for h in range(heads_c):
        o_send(h).wait_send()
        kv_forward(h).wait_send()
        for side in range(2):
            kv_send(h, side).wait_send()
    x_send.wait_send()

    @pl.loop(1, n)
    def _(off):
        tw_send(off).wait_send()


def build_kernel(n, step, hg_ref, pick, wcol, h_ref, buf_ref, stage, h_sem, b_sem):
    nch, toks, col = hg_ref.shape
    sd = toks // n
    per = buf_ref.shape[0]
    rows = pick.shape[1]
    cap = rows // per
    me = lax.axis_index("sp")

    def ds(i, size):
        return pl.ds(pl.multiple_of(i, size), size)

    def h_copy(c):
        return pltpu.make_async_copy(hg_ref.at[c, ds(me * sd, sd)], h_ref.at[:, ds(c * col, col)], h_sem.at[c])

    def b_copy(i, slot):
        return pltpu.make_async_copy(stage.at[slot], buf_ref.at[:, :, ds(i * (step * col), step * col)], b_sem.at[slot])

    @pl.loop(0, nch)
    def _(c):
        h_copy(c).start()

    slots = stage.shape[0]

    @pl.loop(0, nch // step)
    def _(i):
        slot = lax.rem(i, slots)

        @pl.when(i >= slots)
        def _():
            b_copy(i, slot).wait()

        for k in range(step):
            for s in range(n):
                r = jnp.dot(pick[s], hg_ref[i * step + k, s * sd:(s + 1) * sd, :], preferred_element_type=F32)
                w = jnp.concatenate([wcol[s]] * (col // sd), axis=1)
                r = (w * r).astype(BF16)
                for e in range(per):
                    stage[slot, e, s * cap:(s + 1) * cap, k * col:(k + 1) * col] = r[e * cap:(e + 1) * cap]
        b_copy(i, slot).start()

    for k in range(slots):
        b_copy(0, k).wait()

    @pl.loop(0, nch)
    def _(c):
        h_copy(c).wait()


def solution(mesh):
    n = mesh.shape["sp"]
    row = P(("dp", "sp"), None)
    full = P(None, None)

    def local(x, wq, wk, wv, wo, idx, probs):
        sd, hid = x.shape
        heads = wq.shape[1] // HEAD
        kvh = wk.shape[1] // HEAD
        m = heads // kvh
        ne = probs.shape[1]
        per = ne // n
        cap = 2 * sd * idx.shape[1] // ne
        rows = per * cap
        chips = n // CORES
        ct = CORES * sd
        hc = kvh // CORES
        no = hid // CORES // COL
        nq = hc * m * HEAD // COL
        nb = 6
        dma = pltpu.SemaphoreType.DMA
        any_ = pl.BlockSpec(memory_space=pl.ANY)
        vm = pl.BlockSpec(memory_space=pltpu.VMEM)
        hg, pick, wcol = pl.pallas_call(
            functools.partial(block_kernel, n, kvh, m, nb),
            out_shape=(pltpu.VMEM((CORES * no, n * sd, COL), BF16),
                       pltpu.VMEM((n, rows, sd), BF16),
                       pltpu.VMEM((n, rows, sd), F32)),
            in_specs=[any_] * 8,
            out_specs=(any_, vm, vm),
            scratch_shapes=[
                pltpu.VMEM((ct, hid), BF16),
                pltpu.VMEM((nb, hid, COL), BF16),
                pltpu.VMEM((2, ct, HEAD), F32),
                pltpu.VMEM((chips, hc, 2 * ct, HEAD), BF16),
                pltpu.VMEM((nq, HEAD, COL // HEAD * ct), BF16),
                pltpu.VMEM((kvh, ct, m * HEAD), BF16),
                pltpu.VMEM((no, ct, COL), BF16),
                pltpu.VMEM((m * HEAD // COL, chips, ct, COL // HEAD * ct), F32),
                pltpu.VMEM((ct, COL), F32),
                pltpu.VMEM((n, 8, rows), F32),
                pltpu.VMEM((n, 8, rows), F32),
                pltpu.VMEM(idx.shape[::-1], jnp.int32),
                pltpu.VMEM(probs.shape[::-1], F32),
                dma((nb,)), dma((6,)), dma((n,)), dma((n,)),
                dma((2, hc)), dma((hc,)), dma((3, hc)), dma((hc,)), dma((hc,)),
                dma((no,)), dma((3, no)), dma((2, no)), dma((3, no)), dma((3, no)), dma((4, no)),
            ],
            compiler_params=pltpu.CompilerParams(collective_id=0, has_side_effects=True,
                                                 vmem_limit_bytes=50_000_000),
        )(*(pltpu.with_memory_space_constraint(a, pltpu.HBM)
            for a in (x, wq, wk, wv, wo, idx.T, probs.T, jnp.asarray(rope_table(n * sd)))))

        step = 3
        h, buf = pl.pallas_call(
            functools.partial(build_kernel, n, step),
            out_shape=(jax.ShapeDtypeStruct((sd, hid), BF16),
                       jax.ShapeDtypeStruct((per, n * cap, hid), BF16)),
            in_specs=[vm, vm, vm],
            out_specs=(any_, any_),
            scratch_shapes=[pltpu.VMEM((3, per, n * cap, step * COL), BF16),
                            dma((CORES * no,)), dma((3,))],
            compiler_params=pltpu.CompilerParams(vmem_limit_bytes=30_000_000),
        )(hg, pick, wcol)
        return h, buf

    return jax.shard_map(local, mesh=mesh, in_specs=(row, full, full, full, full, row, row), out_specs=(row, P(("dp", "sp"), None, None)), check_vma=False)
```

```python
import functools
import math
import numpy as np
import jax
import jax.numpy as jnp
from jax import lax
from jax.experimental import pallas as pl
from jax.experimental.pallas import tpu as pltpu
from jax.sharding import PartitionSpec as P

HEAD = 128
ROPE_BASE = 1000000.0
CORES = 2
SHIFT = 1
COL = 256
F32 = jnp.float32
BF16 = jnp.bfloat16
MESH = pl.DeviceIdType.MESH


def rope_table(length):
    inv = ROPE_BASE ** (-np.arange(HEAD // 2, dtype=np.float64) * (2.0 / HEAD))
    ang = np.arange(length, dtype=np.float64)[:, None] * inv[None, :]
    c, s = np.cos(ang), np.sin(ang)
    return np.stack([np.concatenate([c, c], 1), np.concatenate([-s, s], 1)]).astype(np.float32)


def block_kernel(n, kvh, m, nb, x_ref, wq_ref, wk_ref, wv_ref, wo_ref, idx_ref, probs_ref, rope_ref,
                 hg_ref, pick_ref, wcol_ref,
                 xf, wbuf, cs, kvb, qt, of, ho, st, accs, tw_own, tw_all, idx_v, probs_v,
                 w_sem, x_sem, tws_sem, twr_sem, kvs_sem, kvf_sem, kvr_sem, os_sem, or_sem,
                 hl_sem, hs_sem, hf_sem, hp_sem, hr_sem, pr_sem):
    sd, hid = x_ref.shape
    chips = n // CORES
    ct = CORES * sd
    heads_c = kvh // CORES
    nk = heads_c * HEAD // COL
    nq = heads_c * m * HEAD // COL
    no = hid // CORES // COL
    hpc = COL // HEAD
    me = lax.axis_index("sp")
    chip = lax.div(me, CORES)
    core = lax.rem(me, CORES)
    partner = me + 1 - 2 * core
    right = lax.rem(me + CORES, n)
    left = lax.rem(me + n - CORES, n)
    rchip = lax.rem(chip + 1, chips)
    lchip = lax.rem(chip + chips - 1, chips)
    fchip = lax.rem(chip + 2, chips)

    def ds(i, size):
        return pl.ds(pl.multiple_of(i, size), size)

    def wcopy(src, col0, slot):
        return pltpu.make_async_copy(src.at[:, ds(col0, COL)], wbuf.at[slot], w_sem.at[slot])

    def k_copy(i, slot):
        return wcopy(wk_ref, core * (heads_c * HEAD) + i * COL, slot)

    def v_copy(i, slot):
        return wcopy(wv_ref, core * (heads_c * HEAD) + i * COL, slot)

    def q_copy(i, slot):
        return wcopy(wq_ref, core * (nq * COL) + i * COL, slot)

    def o_copy(i, slot):
        return wcopy(wo_ref, core * (no * COL) + i * COL, slot)

    base_q = 2 * nk

    def fetch(g):
        slot = lax.rem(g, nb)

        @pl.when(g < base_q + nq)
        def _():
            q_copy(g - base_q, slot).start()

        @pl.when(jnp.logical_and(g >= base_q + nq, g < base_q + nq + no))
        def _():
            o_copy(g - base_q - nq, slot).start()

    own_x = pltpu.make_async_copy(x_ref, xf.at[ds(core * sd, sd)], x_sem.at[2])
    own_x.start()
    rope_cp = pltpu.make_async_copy(rope_ref.at[:, ds(chip * ct, ct)], cs, x_sem.at[3])
    rope_cp.start()
    idx_cp = pltpu.make_async_copy(idx_ref, idx_v, x_sem.at[4])
    idx_cp.start()
    probs_cp = pltpu.make_async_copy(probs_ref, probs_v, x_sem.at[5])
    probs_cp.start()
    for i in range(nk):
        k_copy(i, 2 * i).start()
        v_copy(i, 2 * i + 1).start()

    barrier = pltpu.get_barrier_semaphore()

    @pl.loop(1, n)
    def _(off):
        pl.semaphore_signal(barrier, inc=1, device_id={"sp": lax.rem(me + off, n)}, device_id_type=MESH)

    pl.semaphore_wait(barrier, n - 1)

    def remote(src, dst, ssem, rsem, dev):
        return pltpu.make_async_remote_copy(src_ref=src, dst_ref=dst, send_sem=ssem, recv_sem=rsem,
                                            device_id={"sp": dev}, device_id_type=MESH)

    x_send = remote(x_ref, xf.at[ds(core * sd, sd)], x_sem.at[0], x_sem.at[1], partner)
    x_send.start()
    for i in range(nb - base_q):
        q_copy(i, base_q + i).start()

    ne = probs_ref.shape[0]
    top = idx_ref.shape[0]
    per = ne // n
    cap = 2 * sd * top // ne
    idx_cp.wait()
    probs_cp.wait()
    probs = probs_v[...]
    ei = lax.broadcasted_iota(jnp.int32, (ne, sd), 0)
    mine = jnp.zeros((ne, sd), F32)
    tot = None
    for c in range(top):
        hot = idx_v[c:c + 1, :] == ei
        mine = jnp.where(hot, 1.0, mine)
        sel = jnp.sum(jnp.where(hot, probs, 0.0), axis=0, keepdims=True)
        tot = sel if tot is None else tot + sel
    low = (lax.broadcasted_iota(jnp.int32, (sd, sd), 0) < lax.broadcasted_iota(jnp.int32, (sd, sd), 1))
    rank = jnp.dot(mine.astype(BF16), jnp.where(low, 1.0, 0.0).astype(BF16), preferred_element_type=F32)
    rank = jnp.where(mine > 0.5, rank, -1.0).T
    gate = (probs / tot).T
    rows = per * cap
    lane = lax.broadcasted_iota(jnp.int32, (sd, rows), 1)
    tok1 = (lax.broadcasted_iota(jnp.int32, (sd, rows), 0) + 1).astype(F32)
    sub = lax.broadcasted_iota(jnp.int32, (8, rows), 0)
    for d in range(n):
        rk = jnp.broadcast_to(rank[:, per * d:per * d + 1], (sd, rows))
        gt = jnp.broadcast_to(gate[:, per * d:per * d + 1], (sd, rows))
        for k in range(1, per):
            rk = jnp.where(lane >= k * cap, rank[:, per * d + k:per * d + k + 1], rk)
            gt = jnp.where(lane >= k * cap, gate[:, per * d + k:per * d + k + 1], gt)
        hit = rk == lax.rem(lane, cap).astype(F32)
        t_row = jnp.sum(jnp.where(hit, tok1, 0.0), axis=0, keepdims=True) - 1.0
        w_row = jnp.sum(jnp.where(hit, gt, 0.0), axis=0, keepdims=True)
        tw_own[d] = jnp.where(sub == 0, t_row, jnp.where(sub == 1, w_row, 0.0))
    tw_own_local = pltpu.make_async_copy(tw_own.at[me], tw_all.at[me], twr_sem.at[me])
    tw_own_local.start()

    def tw_send(off):
        d = lax.rem(me + off, n)
        return remote(tw_own.at[d], tw_all.at[me], tws_sem.at[d], twr_sem.at[me], d)

    @pl.loop(1, n)
    def _(off):
        tw_send(off).start()

    own_x.wait()
    rope_cp.wait()
    x_send.wait_recv()

    def rope(t):
        return t * cs[0] + pltpu.roll(t, HEAD // 2, 1) * cs[1]

    def kv_send(h, side):
        dev = right if side == 0 else left
        return remote(kvb.at[chip, h], kvb.at[chip, h], kvs_sem.at[side, h], kvr_sem.at[side, h], dev)

    def kv_forward(h):
        even = h % 2 == 0
        src = lchip if even else rchip
        dev = right if even else left
        return remote(kvb.at[src, h], kvb.at[src, h], kvf_sem.at[h], kvr_sem.at[2, h], dev)

    @pl.loop(0, nk)
    def _(i):
        k_copy(0, 2 * i).wait()
        v_copy(0, 2 * i + 1).wait()
        ka = jnp.dot(xf[...], wbuf[2 * i], preferred_element_type=F32)
        va = jnp.dot(xf[...], wbuf[2 * i + 1], preferred_element_type=F32)
        for hh in range(hpc):
            kvb[chip, hpc * i + hh, 0:ct] = rope(ka[:, hh * HEAD:(hh + 1) * HEAD]).astype(BF16)
        for hh in range(hpc):
            vt = va[:, hh * HEAD:(hh + 1) * HEAD].T.astype(BF16)
            for b in range(ct // HEAD):
                kvb[chip, hpc * i + hh, ct + b * HEAD:ct + (b + 1) * HEAD] = vt[:, b * HEAD:(b + 1) * HEAD]
        for hh in range(hpc):
            for side in range(2):
                kv_send(hpc * i + hh, side).start()
        fetch(2 * i + nb)
        fetch(2 * i + 1 + nb)

    def q_store(i):
        for hh in range(hpc):
            qt[i, :, hh * ct:(hh + 1) * ct] = rope(accs[:, hh * HEAD:(hh + 1) * HEAD]).T.astype(BF16)

    accs[...] = jnp.zeros_like(accs)
    fwd_at = [nq * 5 // 12 + (nq * 2 // 12) * h for h in range(heads_c)]

    @pl.loop(0, nq)
    def _(i):
        slot = lax.rem(base_q + i, nb)
        q_copy(0, slot).wait()
        q_store(jnp.maximum(i - 1, 0))
        accs[...] = jnp.dot(xf[...], wbuf[slot], preferred_element_type=F32)
        fetch(base_q + i + nb)
        for h in range(heads_c):
            @pl.when(i == fwd_at[h])
            def _(h=h):
                kv_send(h, h % 2).wait_recv()
                kv_forward(h).start()

    q_store(nq - 1)
    ex = math.log2(math.e) / math.sqrt(HEAD)
    wide = hpc * ct
    key_i = lax.broadcasted_iota(jnp.int32, (ct, wide), 0)
    qry_i = lax.rem(lax.broadcasted_iota(jnp.int32, (ct, wide), 1), ct)

    def attend(nc, h):
        cnt = m // hpc
        mx, inv = [None] * cnt, [None] * cnt

        def scores(g):
            q = qt[h * cnt + g]
            for j in range(nc):
                s = jnp.dot(kvb[j, h, 0:ct], q, preferred_element_type=F32)
                if j == nc - 1:
                    s = jnp.where(key_i <= qry_i, s, -jnp.inf)
                st[g, j] = s
                sm = jnp.max(s, axis=0, keepdims=True)
                mx[g] = sm if j == 0 else jnp.maximum(mx[g], sm)

        def soft(g):
            for j in range(nc):
                p = jnp.exp2((st[g, j] - mx[g]) * ex)
                st[g, j] = p
                ps = jnp.sum(p, axis=0, keepdims=True)
                tot = ps if j == 0 else tot + ps
            inv[g] = 1.0 / tot

        def out(g):
            for j in range(nc):
                vt = jnp.concatenate([kvb[j, h, ct + b * HEAD:ct + (b + 1) * HEAD] for b in range(ct // HEAD)], axis=1)
                oj = jnp.dot(vt, (st[g, j] * inv[g]).astype(BF16), preferred_element_type=F32)
                o = oj if j == 0 else o + oj
            o = jnp.concatenate([o[:, k * ct:(k + 1) * ct].T for k in range(hpc)], axis=1)
            of[core * heads_c + h, :, g * COL:(g + 1) * COL] = o.astype(BF16)

        for t in range(cnt + 2):
            if t >= 2:
                out(t - 2)
            if t < cnt:
                scores(t)
            if 1 <= t < cnt + 1:
                soft(t - 1)

    def o_send(h):
        return remote(of.at[core * heads_c + h], of.at[core * heads_c + h], os_sem.at[h], or_sem.at[h], partner)

    @pl.loop(0, heads_c)
    def _(h):
        even = lax.rem(h, 2) == 0
        @pl.when(even)
        def _():
            kv_send(h, 1).wait_recv()

        @pl.when(jnp.logical_not(even))
        def _():
            kv_send(h, 0).wait_recv()

        remote(kvb.at[fchip, h], kvb.at[fchip, h], kvf_sem.at[h], kvr_sem.at[2, h], right).wait_recv()
        for nc in range(1, chips + 1):
            @pl.when(chip == nc - 1)
            def _(nc=nc):
                attend(nc, h)
        o_send(h).start()

    @pl.loop(0, heads_c)
    def _(h):
        pltpu.make_async_copy(of.at[(1 - core) * heads_c + h], of.at[(1 - core) * heads_c + h], or_sem.at[h]).wait()

    def place(c, j, who):
        return hg_ref.at[c * no + j, ds(who * ct, ct)]

    def h_local(j):
        return pltpu.make_async_copy(ho.at[j], place(core, j, chip), hl_sem.at[j])

    def h_send(j, side):
        dev = (right, left, partner)[side]
        return remote(ho.at[j], place(core, j, chip), hs_sem.at[side, j],
                      hr_sem.at[side, j] if side < 2 else pr_sem.at[0, j], dev)

    def h_forward(j, side):
        src = (lchip, rchip)[side]
        dev = (right, left)[side]
        return remote(place(core, j, src), place(core, j, src), hf_sem.at[side, j], hr_sem.at[2, j], dev)

    def h_pass(j, k):
        src = (None, lchip, rchip, fchip)[k]
        return remote(place(core, j, src), place(core, j, src), hp_sem.at[k - 1, j], pr_sem.at[k, j], partner)

    group = m * HEAD

    last = chip == chips - 1
    across = chip == lax.rem(chips + 1, chips)

    def sends_on(j, side):
        kind = lax.rem(j, 2) == side
        late = j >= no - 2 * SHIFT
        return jnp.logical_or(jnp.logical_and(kind, jnp.logical_not(jnp.logical_and(late, last))),
                              jnp.logical_and(late, across))

    @pl.loop(0, no)
    def _(j):
        slot = lax.rem(base_q + nq + j, nb)
        o_copy(0, slot).wait()
        acc = None
        for g in range(kvh):
            t = jnp.dot(of[g], wbuf[slot, g * group:(g + 1) * group], preferred_element_type=F32)
            acc = t if acc is None else acc + t
        xs = xf[:, ds(core * (no * COL) + j * COL, COL)].astype(F32)
        ho[j] = (xs + acc).astype(BF16)
        fetch(base_q + nq + j + nb)
        h_send(j, 0).start()
        h_send(j, 1).start()
        h_send(j, 2).start()
        h_local(j).start()

    tw_own_local.wait()

    @pl.loop(1, n)
    def _(off):
        d = lax.rem(me + off, n)
        pltpu.make_async_copy(tw_own.at[d], tw_all.at[d], twr_sem.at[d]).wait()

    li = lax.broadcasted_iota(jnp.int32, (rows, sd), 1).astype(F32)

    @pl.loop(0, n)
    def _(s):
        t = jnp.broadcast_to(tw_all[s, 0:1, :], (sd, rows)).T
        pick_ref[s] = jnp.where(t == li, 1.0, 0.0).astype(BF16)
        wcol_ref[s] = jnp.broadcast_to(tw_all[s, 1:2, :], (sd, rows)).T

    @pl.loop(0, no)
    def _(j):
        h_send(j, 0).wait_recv()

        @pl.when(sends_on(j, 0))
        def _():
            h_forward(j, 0).start()

        h_pass(j, 1).start()
        h_send(j, 1).wait_recv()

        @pl.when(sends_on(j, 1))
        def _():
            h_forward(j, 1).start()

        h_pass(j, 2).start()

    @pl.loop(0, no)
    def _(j):
        h_forward(j, 0).wait_recv()
        h_pass(j, 3).start()

    @pl.loop(0, no)
    def _(j):
        for side in range(3):
            h_send(j, side).wait_send()
        h_local(j).wait()
        for side in range(2):
            @pl.when(sends_on(j, side))
            def _(side=side):
                h_forward(j, side).wait_send()
        for k in range(1, 4):
            h_pass(j, k).wait_send()
        for k in range(4):
            pltpu.make_async_copy(ho.at[j], place(core, j, chip), pr_sem.at[k, j]).wait()

    for h in range(heads_c):
        o_send(h).wait_send()
        kv_forward(h).wait_send()
        for side in range(2):
            kv_send(h, side).wait_send()
    x_send.wait_send()

    @pl.loop(1, n)
    def _(off):
        tw_send(off).wait_send()


def build_kernel(n, step, hg_ref, pick, wcol, h_ref, buf_ref, stage, h_sem, b_sem):
    nch, toks, col = hg_ref.shape
    sd = toks // n
    per = buf_ref.shape[0]
    rows = pick.shape[1]
    cap = rows // per
    me = lax.axis_index("sp")

    def ds(i, size):
        return pl.ds(pl.multiple_of(i, size), size)

    def h_copy(c):
        return pltpu.make_async_copy(hg_ref.at[c, ds(me * sd, sd)], h_ref.at[:, ds(c * col, col)], h_sem.at[c])

    def b_copy(i, slot):
        return pltpu.make_async_copy(stage.at[slot], buf_ref.at[:, :, ds(i * (step * col), step * col)], b_sem.at[slot])

    @pl.loop(0, nch)
    def _(c):
        h_copy(c).start()

    slots = stage.shape[0]

    @pl.loop(0, nch // step)
    def _(i):
        slot = lax.rem(i, slots)

        @pl.when(i >= slots)
        def _():
            b_copy(i, slot).wait()

        for k in range(step):
            for s in range(n):
                r = jnp.dot(pick[s], hg_ref[i * step + k, s * sd:(s + 1) * sd, :], preferred_element_type=F32)
                w = jnp.concatenate([wcol[s]] * (col // sd), axis=1)
                r = (w * r).astype(BF16)
                for e in range(per):
                    stage[slot, e, s * cap:(s + 1) * cap, k * col:(k + 1) * col] = r[e * cap:(e + 1) * cap]
        b_copy(i, slot).start()

    for k in range(slots):
        b_copy(0, k).wait()

    @pl.loop(0, nch)
    def _(c):
        h_copy(c).wait()


def solution(mesh):
    n = mesh.shape["sp"]
    row = P(("dp", "sp"), None)
    full = P(None, None)

    def local(x, wq, wk, wv, wo, idx, probs):
        sd, hid = x.shape
        heads = wq.shape[1] // HEAD
        kvh = wk.shape[1] // HEAD
        m = heads // kvh
        ne = probs.shape[1]
        per = ne // n
        cap = 2 * sd * idx.shape[1] // ne
        rows = per * cap
        chips = n // CORES
        ct = CORES * sd
        hc = kvh // CORES
        no = hid // CORES // COL
        nq = hc * m * HEAD // COL
        nb = 6
        dma = pltpu.SemaphoreType.DMA
        any_ = pl.BlockSpec(memory_space=pl.ANY)
        vm = pl.BlockSpec(memory_space=pltpu.VMEM)
        hg, pick, wcol = pl.pallas_call(
            functools.partial(block_kernel, n, kvh, m, nb),
            out_shape=(pltpu.VMEM((CORES * no, n * sd, COL), BF16),
                       pltpu.VMEM((n, rows, sd), BF16),
                       pltpu.VMEM((n, rows, sd), F32)),
            in_specs=[any_] * 8,
            out_specs=(any_, vm, vm),
            scratch_shapes=[
                pltpu.VMEM((ct, hid), BF16),
                pltpu.VMEM((nb, hid, COL), BF16),
                pltpu.VMEM((2, ct, HEAD), F32),
                pltpu.VMEM((chips, hc, 2 * ct, HEAD), BF16),
                pltpu.VMEM((nq, HEAD, COL // HEAD * ct), BF16),
                pltpu.VMEM((kvh, ct, m * HEAD), BF16),
                pltpu.VMEM((no, ct, COL), BF16),
                pltpu.VMEM((m * HEAD // COL, chips, ct, COL // HEAD * ct), F32),
                pltpu.VMEM((ct, COL), F32),
                pltpu.VMEM((n, 8, rows), F32),
                pltpu.VMEM((n, 8, rows), F32),
                pltpu.VMEM(idx.shape[::-1], jnp.int32),
                pltpu.VMEM(probs.shape[::-1], F32),
                dma((nb,)), dma((6,)), dma((n,)), dma((n,)),
                dma((2, hc)), dma((hc,)), dma((3, hc)), dma((hc,)), dma((hc,)),
                dma((no,)), dma((3, no)), dma((2, no)), dma((3, no)), dma((3, no)), dma((4, no)),
            ],
            compiler_params=pltpu.CompilerParams(collective_id=0, has_side_effects=True,
                                                 vmem_limit_bytes=50_000_000),
        )(*(pltpu.with_memory_space_constraint(a, pltpu.HBM)
            for a in (x, wq, wk, wv, wo, idx.T, probs.T, jnp.asarray(rope_table(n * sd)))))

        step = 3
        h, buf = pl.pallas_call(
            functools.partial(build_kernel, n, step),
            out_shape=(jax.ShapeDtypeStruct((sd, hid), BF16),
                       jax.ShapeDtypeStruct((per, n * cap, hid), BF16)),
            in_specs=[vm, vm, vm],
            out_specs=(any_, any_),
            scratch_shapes=[pltpu.VMEM((4, per, n * cap, step * COL), BF16),
                            dma((CORES * no,)), dma((4,))],
            compiler_params=pltpu.CompilerParams(vmem_limit_bytes=30_000_000),
        )(hg, pick, wcol)
        return h, buf

    return jax.shard_map(local, mesh=mesh, in_specs=(row, full, full, full, full, row, row), out_specs=(row, P(("dp", "sp"), None, None)), check_vma=False)
```
